32 devices in a mesh: blk: 4 (over x, core), fsdp: 8 (over z, y).
Axes of the slice: x: 2, y: 2, z: 4, core: 2. Of those that a mesh axis runs over, the one named last changes fastest.
Arguments:
- normed: bfloat16 [8, 1024, 2048], P('fsdp', 'blk'), may hold values from -128 to 128
- picked: int32 [8, 64], P('fsdp', 'blk'), may hold values from 0 to 255, as said below
- queries: bfloat16 [8, 64, 2048], P('fsdp', 'blk'), may hold values from -9 to 9
- key_states: bfloat16 [8, 1024, 512], P('fsdp', 'blk'), may hold values from -4 to 4
- values: bfloat16 [8, 1024, 512], P('fsdp', 'blk'), may hold values from -6 to 6
- cotangent: bfloat16 [8, 64, 2048], P('fsdp', 'blk'), may hold values from -16 to 16
- hessian: float32 [2048, 512], P(('blk', 'fsdp')), may hold values from 0.1 to 1
Outputs:
- hessian_next: float32 [2048, 512], P(('blk', 'fsdp'))
The draws below stay inside these ranges and needn't reach their ends.
Inputs may be any that keep to these rules, and one draw needn't show every extreme that they name: `picked`: ascending and distinct within each block of 16 rows.
All inputs are finite; a program needn't handle non-finite values.
Results may differ from the reference program's by a relative error of at most 0.007.
Values may be sent and summed in bfloat16 or wider, within the bound.
No kernel may reach another device: no remote copies, remote signals or barrier semaphores. Data moves between devices by JAX's collectives and lax.ppermute only.
A program may use at most 64 MiB of HBM per device.

```python
import math
import jax
import jax.numpy as jnp
from jax import lax

D = 2048
HEADS = 16
KV_HEADS = 4
HEAD_DIM = 128
TOK_DEV = 256
Q_DEV = 16
SEQ = 1024
BATCH = 8
N_BLK = 4


def block_offsets(key):
    seeded = jax.random.fold_in(key, 5)
    streams = jax.random.split(seeded, BATCH * N_BLK)
    chosen = jax.vmap(lambda subkey: jax.random.permutation(subkey, TOK_DEV)[:Q_DEV])(streams)
    return jnp.sort(chosen, axis=-1).reshape(BATCH, N_BLK * Q_DEV).astype(jnp.int32)


def draw_picked(key, part):
    return block_offsets(key)


def draw_normed(key, part):
    layout = (BATCH, SEQ, D)
    own_key = jax.random.fold_in(key, 19)
    drawn = jax.random.truncated_normal(own_key, -4.0, 4.0, layout, jnp.float32)
    pairing = jax.random.permutation(jax.random.fold_in(key, 17), BATCH * N_BLK).reshape(BATCH, N_BLK)
    row_width = D // (BATCH * N_BLK)
    row_block = jnp.arange(D) // row_width
    token_block = jnp.arange(SEQ) // TOK_DEV
    target = pairing[:, token_block]
    boost = jnp.where(target[:, :, None] == row_block[None, None, :], 32.0, 1.0).astype(jnp.float32)
    return (drawn * boost).astype(jnp.bfloat16)


def draw_queries(key, part):
    layout = (BATCH, N_BLK * Q_DEV, KV_HEADS, HEADS // KV_HEADS, HEAD_DIM)
    own_key = jax.random.fold_in(key, 11)
    drawn = jax.random.truncated_normal(own_key, -4.0, 4.0, layout, jnp.float32)
    return drawn.reshape(BATCH, N_BLK * Q_DEV, HEADS * HEAD_DIM).astype(jnp.bfloat16)


def draw_key_states(key, part):
    layout = (BATCH, SEQ, KV_HEADS, HEAD_DIM)
    own_key = jax.random.fold_in(key, 13)
    drawn = jax.random.truncated_normal(own_key, -4.0, 4.0, layout, jnp.float32)
    return drawn.reshape(BATCH, SEQ, KV_HEADS * HEAD_DIM).astype(jnp.bfloat16)


def block_levels(stream_key, shape, pieces, least, high):
    gain = 1.0
    for position, parts in pieces:
        heights = jax.random.uniform(jax.random.fold_in(jax.random.fold_in(stream_key, 6), position), (parts,), jnp.float32, least / len(pieces), high / len(pieces))
        gain = gain * jnp.repeat(jnp.exp(heights), shape[position] // parts).reshape((-1,) + (1,) * (len(shape) - 1 - position))
    return gain


def bell_draw(rng, extent, scale, bound, pieces=(), held_as=jnp.bfloat16):
    values = scale * jax.random.normal(rng, extent, jnp.float32)
    if pieces:
        values = values * block_levels(rng, extent, pieces, -0.22, 0.18)
    return jnp.clip(values, -bound, bound).astype(held_as)


def setup_inputs(seed: int = 0) -> dict:
    arg_keys = jax.random.split(jax.random.key(seed), 8)
    normed = draw_normed(jax.random.fold_in(arg_keys[7], 71), 0)
    picked = draw_picked(jax.random.fold_in(arg_keys[7], 71), 0)
    queries = draw_queries(jax.random.fold_in(arg_keys[7], 71), 0)
    key_states = draw_key_states(jax.random.fold_in(arg_keys[7], 71), 0)
    values = bell_draw(arg_keys[4], (BATCH, SEQ, KV_HEADS * HEAD_DIM), 1.0, 6.0, ((0, 8), (1, 4)))
    cotangent = bell_draw(arg_keys[5], (BATCH, N_BLK * Q_DEV, HEADS * HEAD_DIM), 4.0, 16.0, ((0, 8), (1, 4)))
    hessian = jnp.clip(jnp.exp(math.log(1.0) - 2.3025851 * jax.random.uniform(arg_keys[6], (D, KV_HEADS * HEAD_DIM), jnp.float32) ** block_levels(arg_keys[6], (D, KV_HEADS * HEAD_DIM), ((0, 32),), -0.2, 0.2)), 0.1, 1.0)
    return {"normed": normed, "picked": picked, "queries": queries, "key_states": key_states, "values": values, "cotangent": cotangent, "hessian": hessian}


decay_rate = 0.99
rope_base = 500000.0
neg_large = -1.0e30


def rotate_back(gradient, positions):
    half_dim = gradient.shape[-1] // 2
    exponent = jnp.arange(half_dim, dtype=jnp.float32) * (2.0 / gradient.shape[-1])
    frequency = jnp.power(jnp.float32(rope_base), -exponent)
    angles = positions.astype(jnp.float32)[:, None] * frequency[None, :]
    cosine = jnp.cos(angles)[:, None, :]
    sine_part = jnp.sin(angles)[:, None, :]
    leading = gradient[..., :half_dim]
    trailing = gradient[..., half_dim:]
    return jnp.concatenate([leading * cosine + trailing * sine_part, trailing * cosine - leading * sine_part], axis=-1)


def group_gradient(query_group, key_group, value_group, cot_group, causal):
    scaling = HEAD_DIM ** -0.5
    query_wide = query_group.astype(jnp.float32)
    key_wide = key_group.astype(jnp.float32)
    value_wide = value_group.astype(jnp.float32)
    cot_wide = cot_group.astype(jnp.float32)
    scores = jnp.einsum('qrd,kd->rqk', query_wide, key_wide) * scaling
    scores = jnp.where(causal[None], scores, neg_large)
    new_max = jnp.max(scores, axis=-1)
    exponent = jnp.exp(scores - new_max[..., None])
    running_sum = jnp.sum(exponent, axis=-1)
    rounded = lax.optimization_barrier(exponent.astype(jnp.bfloat16)).astype(jnp.float32)
    attended = jnp.einsum('rqk,kd->rqd', rounded, value_wide) / running_sum[..., None]
    log_norm = new_max + jnp.log(running_sum)
    row_dot = jnp.einsum('qrd,rqd->rq', cot_wide, attended)
    attention = jnp.exp(scores - log_norm[..., None])
    grad_weights = jnp.einsum('qrd,kd->rqk', cot_wide, value_wide)
    grad_scores = attention * (grad_weights - row_dot[..., None])
    grad_scores = lax.optimization_barrier(grad_scores.astype(jnp.bfloat16)).astype(jnp.float32)
    return jnp.einsum('rqk,qrd->kd', grad_scores, query_wide) * scaling


def sequence_gradient(picked_seq, query_seq, key_seq, value_seq, cot_seq):
    length = key_seq.shape[0]
    query_rows = query_seq.shape[0]
    repeat_count = HEADS // KV_HEADS
    positions = (jnp.arange(query_rows, dtype=jnp.int32) // Q_DEV) * TOK_DEV + picked_seq.astype(jnp.int32)
    causal = jnp.arange(length, dtype=jnp.int32)[None, :] <= positions[:, None]
    query_groups = jnp.moveaxis(query_seq.reshape(query_rows, KV_HEADS, repeat_count, HEAD_DIM), 1, 0)
    cot_groups = jnp.moveaxis(cot_seq.reshape(query_rows, KV_HEADS, repeat_count, HEAD_DIM), 1, 0)
    key_groups = jnp.moveaxis(key_seq.reshape(length, KV_HEADS, HEAD_DIM), 1, 0)
    value_groups = jnp.moveaxis(value_seq.reshape(length, KV_HEADS, HEAD_DIM), 1, 0)

    def one_group(packed):
        return group_gradient(packed[0], packed[1], packed[2], packed[3], causal)

    per_group = lax.map(one_group, (query_groups, key_groups, value_groups, cot_groups))
    gradient = jnp.moveaxis(per_group, 0, 1)
    unrotated = rotate_back(gradient, jnp.arange(length, dtype=jnp.int32))
    return unrotated.reshape(length, KV_HEADS * HEAD_DIM).astype(jnp.bfloat16)


def reference(normed, picked, queries, key_states, values, cotangent, hessian):
    def accumulate(running, packed):
        normed_seq, picked_seq, query_seq, key_seq, value_seq, cot_seq = packed
        unrotated = sequence_gradient(picked_seq, query_seq, key_seq, value_seq, cot_seq)
        return running + jnp.dot(normed_seq.T, unrotated, preferred_element_type=jnp.float32), None

    starting = jnp.zeros((D, KV_HEADS * HEAD_DIM), jnp.float32)
    grad_sum, ignored = lax.scan(accumulate, starting, (normed, picked, queries, key_states, values, cotangent))
    return decay_rate * hessian + (1.0 - decay_rate) * grad_sum * grad_sum / BATCH
```

```python
import functools

import jax
import jax.numpy as jnp
from jax import lax
from jax.experimental import pallas as pl
from jax.experimental.pallas import tpu as pltpu
from jax.sharding import PartitionSpec as P

HEADS = 16
KV_HEADS = 4
HEAD_DIM = 128
REPEAT = HEADS // KV_HEADS

decay_rate = 0.99
rope_base = 500000.0
neg_large = -1e30

VMEM = pl.BlockSpec(memory_space=pltpu.VMEM)
SMEM = pl.BlockSpec(memory_space=pltpu.SMEM)
NT_DIMS = (((1,), (1,)), ((), ()))


def swapped(block, axis, bits):
    route = [(i, i ^ bits) for i in range(lax.axis_size(axis))]
    return lax.ppermute(block, axis, route)


def call(kernel, out_shape, in_specs, flops, scratch=()):
    return pl.pallas_call(
        kernel,
        out_shape=out_shape,
        in_specs=in_specs,
        out_specs=jax.tree.map(lambda _: VMEM, out_shape),
        scratch_shapes=scratch,
        cost_estimate=pl.CostEstimate(flops=flops, bytes_accessed=1 << 20, transcendentals=0),
    )


def rotation_tables(first, tokens):
    half = HEAD_DIM // 2
    exponent = jnp.arange(half, dtype=jnp.float32) * (2.0 / HEAD_DIM)
    frequency = jnp.power(jnp.float32(rope_base), -exponent)
    positions = first + lax.broadcasted_iota(jnp.int32, (tokens,), 0)
    angles = positions.astype(jnp.float32)[:, None] * frequency[None, :]
    cosine, sine = jnp.cos(angles), jnp.sin(angles)
    return jnp.concatenate([cosine, cosine], -1), jnp.concatenate([sine, -sine], -1)


def chunks(rows):
    per = max(1, min(REPEAT, 256 // rows))
    return per, REPEAT // per


def collect(order_ref, refs, held):
    rows = refs[0].shape[0]
    for number, ref in enumerate(refs):
        held[pl.ds(pl.multiple_of(order_ref[number] * rows, rows), rows), :] = ref[...]


def heads_of(held, first, count):
    parts = [held[:, pl.ds((first + r) * HEAD_DIM, HEAD_DIM)] for r in range(count)]
    return parts[0] if count == 1 else jnp.concatenate(parts, axis=0)


def stats_kernel(blocks, order_ref, *refs):
    query_refs, cot_refs = refs[:blocks], refs[blocks : 2 * blocks]
    key_ref, value_ref, reach_ref, stats_ref, query_held, cot_held = refs[2 * blocks :]
    collect(order_ref, query_refs, query_held)
    collect(order_ref, cot_refs, cot_held)
    per, count = chunks(query_held.shape[0])
    width = per * query_held.shape[0]
    groups = key_ref.shape[1] // HEAD_DIM
    for group in range(groups):
        columns = pl.ds(group * HEAD_DIM, HEAD_DIM)
        for chunk in range(count):
            first = group * REPEAT + chunk * per
            query = heads_of(query_held, first, per)
            cot = heads_of(cot_held, first, per)
            scores = lax.dot_general(
                key_ref[:, columns], query, NT_DIMS, preferred_element_type=jnp.float32
            ) * (HEAD_DIM**-0.5)
            grads = lax.dot_general(
                value_ref[:, columns], cot, NT_DIMS, preferred_element_type=jnp.float32
            )
            key_ids = lax.broadcasted_iota(jnp.int32, scores.shape, 0)
            scores = jnp.where(key_ids <= reach_ref[...], scores, neg_large)
            top = jnp.max(scores, axis=0, keepdims=True)
            expo = jnp.exp(scores - top)
            total = jnp.sum(expo, axis=0, keepdims=True)
            weights = expo.astype(jnp.bfloat16).astype(jnp.float32)
            dot = jnp.sum(weights * grads, axis=0, keepdims=True)
            place = pl.ds(chunk * width, width)
            stats_ref[0, group : group + 1, place] = top
            stats_ref[1, group : group + 1, place] = total
            stats_ref[2, group : group + 1, place] = dot


def grad_kernel(blocks, order_ref, *refs):
    query_refs, cot_refs = refs[:blocks], refs[blocks : 2 * blocks]
    key_ref, value_ref, reach_ref, norm_ref, dot_ref, cosine_ref, sine_ref = refs[
        2 * blocks : 2 * blocks + 7
    ]
    out_ref, query_held, cot_held = refs[2 * blocks + 7 :]
    collect(order_ref, query_refs, query_held)
    collect(order_ref, cot_refs, cot_held)
    per, count = chunks(query_held.shape[0])
    width = per * query_held.shape[0]
    groups = key_ref.shape[1] // HEAD_DIM
    for group in range(groups):
        columns = pl.ds(group * HEAD_DIM, HEAD_DIM)
        gradient = None
        for chunk in range(count):
            first = group * REPEAT + chunk * per
            query = heads_of(query_held, first, per)
            cot = heads_of(cot_held, first, per)
            place = pl.ds(chunk * width, width)
            scores = lax.dot_general(
                key_ref[:, columns], query, NT_DIMS, preferred_element_type=jnp.float32
            ) * (HEAD_DIM**-0.5)
            grads = lax.dot_general(
                value_ref[:, columns], cot, NT_DIMS, preferred_element_type=jnp.float32
            )
            key_ids = lax.broadcasted_iota(jnp.int32, scores.shape, 0)
            scores = jnp.where(key_ids <= reach_ref[...], scores, neg_large)
            prob = jnp.exp(scores - norm_ref[group : group + 1, place])
            pulled = (prob * (grads - dot_ref[group : group + 1, place])).astype(jnp.bfloat16)
            term = jnp.dot(pulled, query, preferred_element_type=jnp.float32)
            gradient = term if gradient is None else gradient + term
        gradient = gradient * (HEAD_DIM**-0.5)
        turned = pltpu.roll(gradient, HEAD_DIM // 2, 1)
        out_ref[:, columns] = (gradient * cosine_ref[...] + turned * sine_ref[...]).astype(
            jnp.bfloat16
        )


def split_kernel(place_ref, features_ref, keep_ref, send_ref):
    core = place_ref[0]
    rows = keep_ref.shape[0] // 16
    for side in range(2):
        for target, out_ref in ((core, keep_ref), (1 - core, send_ref)):
            start = pl.multiple_of((side * 2 + target) * 8 * rows, 128)
            part = features_ref[:, pl.ds(start, 8 * rows)].T
            for z in range(4):
                for y in range(2):
                    out_ref[pl.ds((side * 8 + y * 4 + z) * rows, rows), :] = part[
                        (z * 2 + y) * rows : (z * 2 + y + 1) * rows
                    ]


def product_kernel(
    place_ref, own_ref, far_ref, own_unrot, far_unrot, a_keep, a_send, b_keep, b_send
):
    side, y = place_ref[1], place_ref[2]
    half = own_ref.shape[0] // 2
    quarter = half // 2
    left = own_unrot.shape[1] // 2

    def product(start, size, columns):
        at = pl.ds(pl.multiple_of(start, quarter), size)
        return jnp.dot(
            own_ref[at, :], own_unrot[:, columns], preferred_element_type=jnp.float32
        ) + jnp.dot(far_ref[at, :], far_unrot[:, columns], preferred_element_type=jnp.float32)

    first, second = pl.ds(0, left), pl.ds(left, left)
    a_send[...] = product((1 - side) * half, half, first).astype(jnp.bfloat16)
    for x in range(2):
        at = pl.ds(x * quarter, quarter)
        b_send[at, :] = product(x * half + (1 - y) * quarter, quarter, second).astype(jnp.bfloat16)
    a_keep[...] = product(side * half, half, first)
    for x in range(2):
        at = pl.ds(x * quarter, quarter)
        b_keep[at, :] = product(x * half + y * quarter, quarter, second)


def gathered_over_blk(query, cot):
    size = lax.axis_size("blk")
    held = {0: (query, cot)}
    bit = size // 2
    while bit:
        for number in sorted(held):
            block = held[number]
            held[number | bit] = tuple(swapped(part, "blk", bit) for part in block)
        bit //= 2
    return [held[number][0] for number in range(size)], [held[number][1] for number in range(size)]


def combined(stats):
    bit = lax.axis_size("blk") // 2
    while bit:
        other = swapped(stats, "blk", bit)
        top = jnp.maximum(stats[0], other[0])
        mine, theirs = jnp.exp(stats[0] - top), jnp.exp(other[0] - top)
        stats = jnp.stack(
            [top, stats[1] * mine + other[1] * theirs, stats[2] * mine + other[2] * theirs]
        )
        bit //= 2
    return stats[0] + jnp.log(stats[1]), stats[2] / stats[1]


def pick(array, index):
    return lax.dynamic_index_in_dim(array, index, 0, keepdims=False)


def reduced_by_halves(unrotated, own, far, place):
    _, side, y = place
    z = lax.axis_index("fsdp") // 2
    far_unrotated = swapped(unrotated, "blk", 1)
    total, width = own.shape[0], unrotated.shape[1]
    half, quarter, left = total // 2, total // 4, width // 2
    shapes = [
        jax.ShapeDtypeStruct((half, left), dtype)
        for dtype in (jnp.float32, jnp.bfloat16, jnp.float32, jnp.bfloat16)
    ]
    a_keep, a_send, b_keep, b_send = call(
        product_kernel, shapes, [SMEM] + [VMEM] * 4, 4 * total * width * own.shape[1]
    )(jnp.stack(place), own, far, unrotated, far_unrotated)
    a_come = swapped(a_send, "blk", 2)
    b_come = swapped(b_send, "fsdp", 1)
    a_sum = (a_keep + a_come.astype(jnp.float32)).reshape(2, quarter, left)
    a_come = swapped(pick(a_sum, 1 - y).astype(jnp.bfloat16), "fsdp", 1)
    b_sum = (b_keep + b_come.astype(jnp.float32)).reshape(2, quarter, left)
    b_come = swapped(pick(b_sum, 1 - side).astype(jnp.bfloat16), "blk", 2)
    a_sum = pick(a_sum, y) + a_come.astype(jnp.float32)
    b_sum = pick(b_sum, side) + b_come.astype(jnp.float32)
    rows = quarter // 4
    both = jnp.concatenate([a_sum, b_sum], axis=-1).reshape(4, rows, width)
    result = pick(both, z)
    for distance in (1, 2, 3):
        route = [(i, (i + 2 * distance) % 8) for i in range(8)]
        piece = pick(both, (z + distance) % 4).astype(jnp.bfloat16)
        result = result + lax.ppermute(piece, "fsdp", route).astype(jnp.float32)
    return result


def local(normed, picked, queries, key_states, values, cotangent, hessian):
    rows = queries.shape[1]
    tokens = key_states.shape[1]
    width = key_states.shape[2]
    groups = width // HEAD_DIM
    blocks, sequences = lax.axis_size("blk"), lax.axis_size("fsdp")
    place_blk = lax.axis_index("blk")
    features = normed[0]
    halves = blocks == 4 and sequences == 8 and hessian.shape[0] == 64 and tokens % 128 == 0

    if blocks & (blocks - 1) == 0:
        query_blocks, cot_blocks = gathered_over_blk(queries[0], cotangent[0])
        order = jnp.arange(blocks, dtype=jnp.int32) ^ place_blk
    else:
        all_queries = lax.all_gather(queries[0], "blk", axis=0)
        all_cots = lax.all_gather(cotangent[0], "blk", axis=0)
        query_blocks = [all_queries[i] for i in range(blocks)]
        cot_blocks = [all_cots[i] for i in range(blocks)]
        order = jnp.arange(blocks, dtype=jnp.int32)

    ids = jnp.arange(blocks, dtype=jnp.int32)[:, None]
    reach = jnp.where(
        ids == place_blk, picked, jnp.where(ids > place_blk, jnp.int32(tokens), jnp.int32(-1))
    ).reshape(1, blocks * rows)
    per, count = chunks(blocks * rows)
    reach = jnp.tile(reach, (1, per))
    cosine, sine = rotation_tables(place_blk * tokens, tokens)

    if halves:
        place = (place_blk % 2, place_blk // 2, lax.axis_index("fsdp") % 2)
        half = jax.ShapeDtypeStruct((features.shape[1] // 2, tokens), jnp.bfloat16)
        own, far = call(split_kernel, [half, half], [SMEM, VMEM], 1 << 27)(
            jnp.stack(place), features
        )
        far = swapped(far, "blk", 1)

    held = pltpu.VMEM((blocks * rows, HEADS * HEAD_DIM), jnp.bfloat16)
    operands = (order, *query_blocks, *cot_blocks, key_states[0], values[0], reach)
    specs = [SMEM] + [VMEM] * (2 * blocks + 3)
    work = 4 * HEADS * blocks * rows * tokens * HEAD_DIM
    stats = call(
        functools.partial(stats_kernel, blocks),
        jax.ShapeDtypeStruct((3, groups, REPEAT * blocks * rows), jnp.float32),
        specs,
        work,
        [held, held],
    )(*operands)
    log_norm, row_dot = combined(stats) if blocks & (blocks - 1) == 0 else gathered_stats(stats)
    unrotated = call(
        functools.partial(grad_kernel, blocks),
        jax.ShapeDtypeStruct((tokens, width), jnp.bfloat16),
        specs + [VMEM] * 4,
        work + work // 2,
        [held, held],
    )(*operands, log_norm, row_dot, cosine, sine)

    if halves:
        summed = reduced_by_halves(unrotated, own, far, place)
    else:
        term = lax.dot_general(
            features, unrotated, (((0,), (0,)), ((), ())), preferred_element_type=jnp.float32
        )
        summed = lax.psum_scatter(term, ("blk", "fsdp"), scatter_dimension=0, tiled=True)
    return decay_rate * hessian + (1.0 - decay_rate) * summed * summed / sequences


def gathered_stats(stats):
    every = lax.all_gather(stats, "blk", axis=0)
    top = jnp.max(every[:, 0], axis=0)
    shrink = jnp.exp(every[:, 0] - top)
    total = jnp.sum(every[:, 1] * shrink, axis=0)
    dot = jnp.sum(every[:, 2] * shrink, axis=0)
    return top + jnp.log(total), dot / total


def solution(mesh):
    placed = (
        P("fsdp", "blk", None),
        P("fsdp", "blk"),
        P("fsdp", "blk", None),
        P("fsdp", "blk", None),
        P("fsdp", "blk", None),
        P("fsdp", "blk", None),
        P(("blk", "fsdp"), None),
    )
    return jax.shard_map(
        local, mesh=mesh, in_specs=placed, out_specs=P(("blk", "fsdp"), None), check_vma=False
    )
```

```python
import functools

import jax
import jax.numpy as jnp
import numpy as np
from jax import lax
from jax.experimental import pallas as pl
from jax.experimental.pallas import tpu as pltpu
from jax.sharding import PartitionSpec as P


HEADS = 16
KV_HEADS = 4
HEAD_DIM = 128
REPEAT = HEADS // KV_HEADS

decay_rate = 0.99
rope_base = 500000.0
neg_large = -1e30

VMEM = pl.BlockSpec(memory_space=pltpu.VMEM)
HBM = pl.BlockSpec(memory_space=pltpu.HBM)
NT_DIMS = (((1,), (1,)), ((), ()))
BOTH = ("blk", "fsdp")


def swapped(block, axis, bits):
    route = [(i, i ^ bits) for i in range(lax.axis_size(axis))]
    return lax.ppermute(block, axis, route)


def call(kernel, out_shape, in_specs, flops, scratch=()):
    return pl.pallas_call(
        kernel,
        out_shape=out_shape,
        in_specs=in_specs,
        out_specs=jax.tree.map(lambda _: VMEM, out_shape),
        scratch_shapes=scratch,
        compiler_params=pltpu.CompilerParams(vmem_limit_bytes=16 << 20),
        cost_estimate=pl.CostEstimate(flops=flops, bytes_accessed=1 << 20, transcendentals=0),
    )


def shape(dims, dtype):
    return jax.ShapeDtypeStruct(dims, dtype)


def rotation_rows(positions):
    half = HEAD_DIM // 2
    frequency = rope_base ** (-2.0 * np.arange(half) / HEAD_DIM)
    angles = positions[:, None] * frequency[None, :]
    cosine, sine = np.cos(angles), np.sin(angles)
    pair = np.concatenate([cosine, cosine], -1), np.concatenate([sine, -sine], -1)
    return jnp.asarray(np.stack(pair).astype(np.float32))


def fill_rotation(starts, tokens, coarse_ref, fine_ref, cosine_ref, sine_ref):
    fine_cos, fine_sin = fine_ref[0], fine_ref[1]
    for part, start in enumerate(starts):
        for step in range(tokens // 16):
            row = pl.ds(start // 16 + step, 1)
            cosine, sine = coarse_ref[0, row, :], coarse_ref[1, row, :]
            at = pl.ds(part * tokens + step * 16, 16)
            cosine_ref[at, :] = cosine * fine_cos - sine * fine_sin
            sine_ref[at, :] = sine * fine_cos + cosine * fine_sin


def position():
    blk, fsdp = lax.axis_index("blk"), lax.axis_index("fsdp")
    return blk & 1, blk >> 1, fsdp & 1, fsdp >> 1


def first_second():
    core, side, y, _ = position()
    return jnp.where(core == 0, side, y), jnp.where(core == 0, y, side)


def chunks(rows):
    per = max(1, min(REPEAT, 256 // rows))
    return per, REPEAT // per


def heads_of(held, first, count):
    parts = [held[:, pl.ds((first + r) * HEAD_DIM, HEAD_DIM)] for r in range(count)]
    return parts[0] if count == 1 else jnp.concatenate(parts, axis=0)


def reach_of(picked, here, width, blocks, tokens):
    rows = picked.shape[1]
    square = (rows, rows)
    diagonal = lax.broadcasted_iota(jnp.int32, square, 0) == lax.broadcasted_iota(
        jnp.int32, square, 1
    )
    column = jnp.sum(jnp.where(diagonal, picked, 0), axis=1, keepdims=True)
    lane = lax.broadcasted_iota(jnp.int32, (rows, width), 1)
    chosen = lax.broadcasted_iota(jnp.int32, (rows, width), 0) == (lane & (rows - 1))
    own = jnp.sum(jnp.where(chosen, column, 0), axis=0, keepdims=True)
    lane = lax.broadcasted_iota(jnp.int32, (1, width), 1)
    block = (lane >> (rows.bit_length() - 1)) & (blocks - 1)
    return jnp.where(block == here, own, jnp.where(block > here, tokens, -1))


def stats_kernel(torus, blocks, parts, *refs):
    query_refs, cot_refs = refs[:blocks], refs[blocks : 2 * blocks]
    key_refs, value_refs = (
        refs[(2 * blocks + i * parts) : (2 * blocks + (i + 1) * parts)] for i in range(2)
    )
    reach_refs = refs[2 * blocks + 2 * parts : 2 * blocks + 3 * parts]
    stats_ref, expo_ref, grads_ref, query_held, cot_held = refs[2 * blocks + 3 * parts :]
    rows, width = query_refs[0].shape[0], query_held.shape[1]
    start = position()[0] * width if torus else 0
    columns = pl.ds(pl.multiple_of(start, HEAD_DIM), width)
    for number in range(blocks):
        block = lax.axis_index("blk") ^ number if torus else number
        at = pl.ds(pl.multiple_of(block * rows, rows), rows)
        query_held[at, :] = query_refs[number][:, columns]
        cot_held[at, :] = cot_refs[number][:, columns]
    per, count = chunks(query_held.shape[0])
    width = per * query_held.shape[0]
    start = position()[0] * (HEAD_DIM * stats_ref.shape[1]) if torus else 0
    for group in range(stats_ref.shape[1]):
        columns = pl.ds(pl.multiple_of(start + group * HEAD_DIM, HEAD_DIM), HEAD_DIM)
        for chunk in range(count):
            first = group * REPEAT + chunk * per
            query = heads_of(query_held, first, per)
            cot = heads_of(cot_held, first, per)
            scores, tops = [], []
            for part in range(parts):
                score = lax.dot_general(
                    key_refs[part][:, columns], query, NT_DIMS, preferred_element_type=jnp.float32
                ) * (HEAD_DIM**-0.5)
                key_ids = lax.broadcasted_iota(jnp.int32, score.shape, 0)
                score = jnp.where(key_ids <= reach_refs[part][...], score, neg_large)
                scores.append(score)
                tops.append(jnp.max(score, axis=0, keepdims=True))
            top = functools.reduce(jnp.maximum, tops)
            place = pl.ds(chunk * width, width)
            total, dot = 0.0, 0.0
            for part in range(parts):
                grads = lax.dot_general(
                    value_refs[part][:, columns], cot, NT_DIMS, preferred_element_type=jnp.float32
                )
                expo = jnp.exp(scores[part] - top)
                weights = expo.astype(jnp.bfloat16).astype(jnp.float32)
                total += jnp.sum(expo, axis=0, keepdims=True)
                dot += jnp.sum(weights * grads, axis=0, keepdims=True)
                expo_ref[group, part, :, place] = expo
                grads_ref[group, part, :, place] = grads
            stats_ref[0, group : group + 1, place] = top
            stats_ref[1, group : group + 1, place] = total
            stats_ref[2, group : group + 1, place] = dot


def attention_stats(queries, cots, keys, values, reach, heads, torus):
    blocks, parts = len(queries), len(keys)
    rows = queries[0].shape[0]
    width = heads * REPEAT * HEAD_DIM
    tokens = keys[0].shape[0]
    total = blocks * rows
    saved = shape((heads, parts, tokens, REPEAT * total), jnp.float32)
    held = shape((total, width), jnp.bfloat16)
    outs = [shape((3, heads, REPEAT * total), jnp.float32), saved, saved, held, held]
    return call(
        functools.partial(stats_kernel, torus, blocks, parts),
        outs,
        [VMEM] * (2 * blocks + 3 * parts),
        4 * heads * REPEAT * total * tokens * parts * HEAD_DIM,
    )(*queries, *cots, *keys, *values, *reach)[:4]


def row_scales(group, mine_ref, every_refs):
    at = slice(group, group + 1)
    top = functools.reduce(jnp.maximum, [ref[0, at, :] for ref in every_refs])
    shrink = [jnp.exp(ref[0, at, :] - top) for ref in every_refs]
    total = sum(ref[1, at, :] * factor for ref, factor in zip(every_refs, shrink))
    dot = sum(ref[2, at, :] * factor for ref, factor in zip(every_refs, shrink))
    return jnp.exp(mine_ref[0, at, :] - top) / total, dot / total


def key_gradient(group, stats_refs, expo_ref, grads_ref, query_ref, cosine_ref, sine_ref):
    scale, dot = row_scales(group, stats_refs[0], stats_refs)
    parts, tokens = expo_ref.shape[1:3]
    per, count = chunks(query_ref.shape[0])
    width = per * query_ref.shape[0]
    blocks = []
    for part in range(parts):
        gradient = 0.0
        for chunk in range(count):
            place = slice(chunk * width, (chunk + 1) * width)
            query = heads_of(query_ref, group * REPEAT + chunk * per, per)
            prob = expo_ref[group, part, :, place] * scale[:, place]
            pulled = prob * (grads_ref[group, part, :, place] - dot[:, place])
            gradient += jnp.dot(
                pulled.astype(jnp.bfloat16), query, preferred_element_type=jnp.float32
            )
        gradient = gradient * (HEAD_DIM**-0.5)
        turned = pltpu.roll(gradient, HEAD_DIM // 2, 1)
        at = slice(part * tokens, (part + 1) * tokens)
        blocks.append(
            (gradient * cosine_ref[at, :] + turned * sine_ref[at, :]).astype(jnp.bfloat16)
        )
    return blocks


def grad_kernel(count, *refs):
    stats_refs, out_ref = refs[:count], refs[-1]
    for group in range(stats_refs[0].shape[1]):
        blocks = key_gradient(group, stats_refs, *refs[count:-1])
        out_ref[:, group * HEAD_DIM : (group + 1) * HEAD_DIM] = blocks[0]


def send_kernel(group, *refs):
    stats_refs, saved_refs = refs[:2], refs[2:7]
    own_ref, far_ref, unrot_ref, out_ref = refs[7:]
    own, far = key_gradient(group, stats_refs, *saved_refs)
    unrot_ref[0] = own
    unrot_ref[1] = far
    half = out_ref.shape[0]
    at = pl.ds(pl.multiple_of((1 - first_second()[0]) * half, half), half)
    out_ref[...] = (
        jnp.dot(own_ref[at, :], own, preferred_element_type=jnp.float32)
        + jnp.dot(far_ref[at, :], far, preferred_element_type=jnp.float32)
    ).astype(jnp.bfloat16)


def keep_kernel(own_ref, far_ref, unrot_ref, out_ref):
    half = out_ref.shape[0]
    at = pl.ds(pl.multiple_of(first_second()[0] * half, half), half)
    out_ref[...] = jnp.dot(
        own_ref[at, :], unrot_ref[0], preferred_element_type=jnp.float32
    ) + jnp.dot(far_ref[at, :], unrot_ref[1], preferred_element_type=jnp.float32)


def halve_kernel(*refs):
    keep_refs, come_refs, (send_ref, hold_ref) = refs[:2], refs[2:4], refs[4:]
    half = hold_ref.shape[0]
    second = first_second()[1]
    for place, out_ref in ((1 - second, send_ref), (second, hold_ref)):
        at = pl.ds(pl.multiple_of(place * half, half), half)
        for head in range(2):
            total = keep_refs[head][at, :] + come_refs[head][at, :].astype(jnp.float32)
            out_ref[:, head * HEAD_DIM : (head + 1) * HEAD_DIM] = total.astype(out_ref.dtype)


def quarter_kernel(hold_ref, come_ref, *outs):
    rows = outs[0].shape[0]
    z = position()[3]
    for distance in (2, 3, 1, 0):
        at = pl.ds(pl.multiple_of(((z + distance) & 3) * rows, rows), rows)
        total = hold_ref[at, :] + come_ref[at, :].astype(jnp.float32)
        outs[distance][...] = total.astype(outs[distance].dtype)


def last_kernel(*refs):
    terms, (here_ref, there_ref) = refs[:4], refs[4:]
    rows = here_ref.shape[0]
    core = position()[0]
    for owner, out_ref in ((1 - core, there_ref), (core, here_ref)):
        at = pl.ds(pl.multiple_of(owner * rows, rows), rows)
        out_ref[...] = sum(ref[at, :].astype(jnp.float32) for ref in terms)


def next_kernel(scale, here_ref, there_ref, hessian_ref, out_ref):
    width = here_ref.shape[1]
    core = position()[0]
    for owner, ref in ((core, here_ref), (1 - core, there_ref)):
        columns = pl.ds(pl.multiple_of(owner * width, width), width)
        term = ref[...]
        out_ref[:, columns] = decay_rate * hessian_ref[:, columns] + scale * term * term


def turn_kernel(features_ref, out_ref):
    rows = out_ref.shape[0] // 32
    core = position()[0]
    for x in range(2):
        for c in range(2):
            part = features_ref[:, pl.ds((x * 2 + c) * 8 * rows, 8 * rows)].T
            for z in range(4):
                for y in range(2):
                    pair = jnp.where(core == 0, x * 2 + y, y * 2 + x)
                    at = pl.multiple_of((pair * 8 + z * 2 + c) * rows, rows)
                    out_ref[pl.ds(at, rows), :] = part[
                        (z * 2 + y) * rows : (z * 2 + y + 1) * rows
                    ]


def own_kernel(blocks, *refs):
    sources, (turned_ref, cosine_ref, sine_ref, reach_ref), rest = refs[:8], refs[8:12], refs[12:]
    held, sems = rest[:-1], rest[-1]
    copies = [
        pltpu.make_async_copy(source, target, sems.at[number])
        for number, (source, target) in enumerate(zip(sources, held))
    ]
    for copy in copies:
        copy.start()
    for copy in copies:
        copy.wait()
    keys_ref, (picked_ref, features_ref, coarse_ref, fine_ref) = held[0], held[4:]
    tokens, blk = keys_ref.shape[0], lax.axis_index("blk")
    reach_ref[...] = reach_of(picked_ref[...], blk, reach_ref.shape[1], blocks, tokens)
    starts = blk * tokens, (blk ^ 1) * tokens
    fill_rotation(starts, tokens, coarse_ref, fine_ref, cosine_ref, sine_ref)
    turn_kernel(features_ref, turned_ref)


def far_kernel(blocks, tokens, features_ref, picked_ref, turned_ref, reach_ref):
    here = lax.axis_index("blk") ^ 1
    reach_ref[...] = reach_of(picked_ref[...], here, reach_ref.shape[1], blocks, tokens)
    turn_kernel(features_ref, turned_ref)


def reduced_on_torus(normed, picked, queries, key_states, values, cotangent, hessian):
    tokens = key_states.shape[0]
    out_rows = hessian.shape[0]
    heads = KV_HEADS // 2

    first = swapped(queries, "blk", 2), swapped(cotangent, "blk", 2)
    second = swapped(queries, "blk", 1), swapped(cotangent, "blk", 1)
    third = swapped(first[0], "blk", 1), swapped(first[1], "blk", 1)
    far_keys, far_values = swapped(key_states, "blk", 1), swapped(values, "blk", 1)
    far_normed, far_picked = swapped(normed, "blk", 1), swapped(picked, "blk", 1)

    coarse, fine = rotation_rows(np.arange(0, 4 * tokens, 16)), rotation_rows(np.arange(16))
    turned = shape((normed.shape[1], tokens), jnp.bfloat16)
    table = shape((2 * tokens, HEAD_DIM), jnp.float32)
    last = shape((1, REPEAT * 4 * queries.shape[0]), jnp.int32)
    given = [
        pltpu.with_memory_space_constraint(array, pltpu.HBM)
        for array in (key_states, values, queries, cotangent, picked, normed, coarse, fine)
    ]
    own, cosine, sine, reach, *fetched = call(
        functools.partial(own_kernel, 4),
        [turned, table, table, last] + [shape(array.shape, array.dtype) for array in given[:4]],
        [HBM] * 8,
        1 << 28,
        [pltpu.VMEM(array.shape, array.dtype) for array in given[4:]]
        + [pltpu.SemaphoreType.DMA((8,))],
    )(*given)
    key_states, values, *held = fetched
    held = [held, second, first, third]
    far, far_reach = call(
        functools.partial(far_kernel, 4, tokens), [turned, last], [VMEM] * 2, 1 << 28
    )(far_normed, far_picked)

    stats, expo, grads, query = attention_stats(
        [pair[0] for pair in held],
        [pair[1] for pair in held],
        [key_states, far_keys],
        [values, far_values],
        (reach, far_reach),
        heads,
        True,
    )
    other = swapped(stats, "blk", 2)

    half_rows = normed.shape[1] // 2
    work = 2 * half_rows * 2 * tokens * HEAD_DIM
    route = [(i, i ^ (1 if (i // 8) % 2 else 16)) for i in range(32)]
    route_after = [(i, i ^ (16 if (i // 8) % 2 else 1)) for i in range(32)]
    keeps, come = [], []
    for group in range(heads):
        unrot, send = call(
            functools.partial(send_kernel, group),
            [shape((2, tokens, HEAD_DIM), jnp.bfloat16), shape((half_rows, HEAD_DIM), jnp.bfloat16)],
            [VMEM] * 9,
            work,
        )(stats, other, expo, grads, query, cosine, sine, own, far)
        come.append(lax.ppermute(send, BOTH, route))
        keeps.append(
            call(keep_kernel, shape((half_rows, HEAD_DIM), jnp.float32), [VMEM] * 3, work)(
                own, far, unrot
            )
        )
    block = half_rows // 2, heads * HEAD_DIM
    send, hold = call(
        halve_kernel, [shape(block, jnp.bfloat16), shape(block, jnp.float32)], [VMEM] * 4, 1 << 20
    )(*keeps, *come)
    come = lax.ppermute(send, BOTH, route_after)
    piece = block[0] // 4, block[1]
    mine, *sends = call(
        quarter_kernel,
        [shape(piece, jnp.float32)] + [shape(piece, jnp.bfloat16)] * 3,
        [VMEM] * 2,
        1 << 20,
    )(hold, come)
    arrived = []
    for distance, send in enumerate(sends, 1):
        along = [(i, (i + 2 * distance) % 8) for i in range(8)]
        arrived.append(lax.ppermute(send, "fsdp", along))
    columns = shape((out_rows, block[1]), jnp.float32)
    here, there = call(last_kernel, [columns] * 2, [VMEM] * 4, 1 << 20)(mine, *arrived)
    there = swapped(there, "blk", 1)
    return call(
        functools.partial(next_kernel, (1.0 - decay_rate) / lax.axis_size("fsdp")),
        shape(hessian.shape, jnp.float32),
        [VMEM] * 3,
        1 << 20,
    )(here, there, hessian)


def reduced_anywhere(normed, picked, queries, key_states, values, cotangent):
    rows, tokens = queries.shape[0], key_states.shape[0]
    size, blk = lax.axis_size("blk"), lax.axis_index("blk")
    every_query = lax.all_gather(queries, "blk", axis=0)
    every_cot = lax.all_gather(cotangent, "blk", axis=0)
    order = jnp.arange(size, dtype=jnp.int32)
    ids = order[:, None]
    reach = jnp.where(
        ids == blk, picked, jnp.where(ids > blk, jnp.int32(tokens), jnp.int32(-1))
    ).reshape(1, size * rows)
    reach = jnp.tile(reach, (1, chunks(size * rows)[0]))
    cosine, sine = lax.dynamic_index_in_dim(
        rotation_rows(np.arange(size * tokens)).reshape(2, size, tokens, HEAD_DIM), blk, 1, False
    )
    stats, expo, grads, query = attention_stats(
        [every_query[i] for i in range(size)],
        [every_cot[i] for i in range(size)],
        [key_states],
        [values],
        (reach,),
        KV_HEADS,
        False,
    )
    gathered = lax.all_gather(stats, "blk", axis=0)
    others = [gathered[(blk + i) % size] for i in range(1, size)]
    unrotated = call(
        functools.partial(grad_kernel, size),
        shape((tokens, KV_HEADS * HEAD_DIM), jnp.bfloat16),
        [VMEM] * (size + 5),
        1 << 28,
    )(stats, *others, expo, grads, query, cosine, sine)
    term = lax.dot_general(
        normed, unrotated, (((0,), (0,)), ((), ())), preferred_element_type=jnp.float32
    )
    return lax.psum_scatter(term, BOTH, scatter_dimension=0, tiled=True)


def on_torus(blocks, sequences):
    return blocks == 4 and sequences == 8


def local(normed, picked, queries, key_states, values, cotangent, hessian):
    given = (normed[0], picked, queries[0], key_states[0], values[0], cotangent[0])
    rows, tokens, out_rows = queries.shape[1], key_states.shape[1], hessian.shape[0]
    blocks, sequences = lax.axis_size("blk"), lax.axis_size("fsdp")
    fits = rows & (rows - 1) == 0 and rows <= 16 and tokens % 128 == 0 and out_rows % 16 == 0
    if on_torus(blocks, sequences):
        assert fits
        return reduced_on_torus(*given, hessian)
    summed = reduced_anywhere(*given)
    return decay_rate * hessian + (1.0 - decay_rate) * summed * summed / sequences


def solution(mesh):
    placed = (
        P("fsdp", "blk", None),
        P("fsdp", "blk"),
        P("fsdp", "blk", None),
        P("fsdp", "blk", None),
        P("fsdp", "blk", None),
        P("fsdp", "blk", None),
        P(("blk", "fsdp"), None),
    )
    return jax.shard_map(
        local, mesh=mesh, in_specs=placed, out_specs=P(("blk", "fsdp"), None), check_vma=False
    )
```

```python
import functools

import jax
import jax.numpy as jnp
import numpy as np
from jax import lax
from jax.experimental import pallas as pl
from jax.experimental.pallas import tpu as pltpu
from jax.sharding import PartitionSpec as P


HEADS = 16
KV_HEADS = 4
HEAD_DIM = 128
REPEAT = HEADS // KV_HEADS

decay_rate = 0.99
rope_base = 500000.0
neg_large = -1e30

VMEM = pl.BlockSpec(memory_space=pltpu.VMEM)
HBM = pl.BlockSpec(memory_space=pltpu.HBM)
NT_DIMS = (((1,), (1,)), ((), ()))
BOTH = ("blk", "fsdp")
TRAVEL, STAY, EARLY = ((1, 2), (3, 0)), ((1, 2), (3, 0)), 2


def swapped(block, axis, bits):
    route = [(i, i ^ bits) for i in range(lax.axis_size(axis))]
    return lax.ppermute(block, axis, route)


def call(kernel, out_shape, in_specs, flops, scratch=()):
    return pl.pallas_call(
        kernel,
        out_shape=out_shape,
        in_specs=in_specs,
        out_specs=jax.tree.map(lambda _: VMEM, out_shape),
        scratch_shapes=scratch,
        compiler_params=pltpu.CompilerParams(vmem_limit_bytes=16 << 20),
        cost_estimate=pl.CostEstimate(flops=flops, bytes_accessed=1 << 20, transcendentals=0),
    )


def shape(dims, dtype):
    return jax.ShapeDtypeStruct(dims, dtype)


def rotation_rows(positions):
    half = HEAD_DIM // 2
    frequency = rope_base ** (-2.0 * np.arange(half) / HEAD_DIM)
    angles = positions[:, None] * frequency[None, :]
    cosine, sine = np.cos(angles), np.sin(angles)
    pair = np.concatenate([cosine, cosine], -1), np.concatenate([sine, -sine], -1)
    return jnp.asarray(np.stack(pair).astype(np.float32))


def fill_rotation(starts, tokens, coarse_ref, fine_ref, cosine_ref, sine_ref):
    fine_cos, fine_sin = fine_ref[0], fine_ref[1]
    for part, start in enumerate(starts):
        for step in range(tokens // 16):
            row = pl.ds(start // 16 + step, 1)
            cosine, sine = coarse_ref[0, row, :], coarse_ref[1, row, :]
            at = pl.ds(part * tokens + step * 16, 16)
            cosine_ref[at, :] = cosine * fine_cos - sine * fine_sin
            sine_ref[at, :] = sine * fine_cos + cosine * fine_sin


def position():
    blk, fsdp = lax.axis_index("blk"), lax.axis_index("fsdp")
    return blk & 1, blk >> 1, fsdp & 1, fsdp >> 1


def first_second():
    core, side, y, _ = position()
    return jnp.where(core == 0, side, y), jnp.where(core == 0, y, side)


def chunks(rows):
    per = max(1, min(REPEAT, 256 // rows))
    return per, REPEAT // per


def heads_of(held, first, count):
    parts = [held[:, pl.ds((first + r) * HEAD_DIM, HEAD_DIM)] for r in range(count)]
    return parts[0] if count == 1 else jnp.concatenate(parts, axis=0)


def reach_of(picked, here, width, blocks, tokens):
    rows = picked.shape[1]
    square = (rows, rows)
    diagonal = lax.broadcasted_iota(jnp.int32, square, 0) == lax.broadcasted_iota(
        jnp.int32, square, 1
    )
    column = jnp.sum(jnp.where(diagonal, picked, 0), axis=1, keepdims=True)
    lane = lax.broadcasted_iota(jnp.int32, (rows, width), 1)
    chosen = lax.broadcasted_iota(jnp.int32, (rows, width), 0) == (lane & (rows - 1))
    own = jnp.sum(jnp.where(chosen, column, 0), axis=0, keepdims=True)
    lane = lax.broadcasted_iota(jnp.int32, (1, width), 1)
    block = (lane >> (rows.bit_length() - 1)) & (blocks - 1)
    return jnp.where(block == here, own, jnp.where(block > here, tokens, -1))


def stats_kernel(torus, blocks, parts, *refs):
    query_refs, cot_refs = refs[:blocks], refs[blocks : 2 * blocks]
    key_refs, value_refs = (
        refs[(2 * blocks + i * parts) : (2 * blocks + (i + 1) * parts)] for i in range(2)
    )
    reach_refs = refs[2 * blocks + 2 * parts : 2 * blocks + 3 * parts]
    stats_ref, expo_ref, grads_ref, query_held, cot_held = refs[2 * blocks + 3 * parts :]
    rows, width = query_refs[0].shape[0], query_held.shape[1]
    start = position()[0] * width if torus else 0
    columns = pl.ds(pl.multiple_of(start, HEAD_DIM), width)
    for number in range(blocks):
        block = lax.axis_index("blk") ^ number if torus else number
        at = pl.ds(pl.multiple_of(block * rows, rows), rows)
        query_held[at, :] = query_refs[number][:, columns]
        cot_held[at, :] = cot_refs[number][:, columns]
    per, count = chunks(query_held.shape[0])
    width = per * query_held.shape[0]
    start = position()[0] * (HEAD_DIM * stats_ref.shape[1]) if torus else 0
    for group in range(stats_ref.shape[1]):
        columns = pl.ds(pl.multiple_of(start + group * HEAD_DIM, HEAD_DIM), HEAD_DIM)
        for chunk in range(count):
            first = group * REPEAT + chunk * per
            query = heads_of(query_held, first, per)
            cot = heads_of(cot_held, first, per)
            scores, tops = [], []
            for part in range(parts):
                score = lax.dot_general(
                    key_refs[part][:, columns], query, NT_DIMS, preferred_element_type=jnp.float32
                ) * (HEAD_DIM**-0.5)
                key_ids = lax.broadcasted_iota(jnp.int32, score.shape, 0)
                score = jnp.where(key_ids <= reach_refs[part][...], score, neg_large)
                scores.append(score)
                tops.append(jnp.max(score, axis=0, keepdims=True))
            top = functools.reduce(jnp.maximum, tops)
            place = pl.ds(chunk * width, width)
            total, dot = 0.0, 0.0
            for part in range(parts):
                grads = lax.dot_general(
                    value_refs[part][:, columns], cot, NT_DIMS, preferred_element_type=jnp.float32
                )
                expo = jnp.exp(scores[part] - top)
                weights = expo.astype(jnp.bfloat16).astype(jnp.float32)
                total += jnp.sum(expo, axis=0, keepdims=True)
                dot += jnp.sum(weights * grads, axis=0, keepdims=True)
                expo_ref[group, part, :, place] = expo
                grads_ref[group, part, :, place] = grads
            stats_ref[0, group : group + 1, place] = top
            stats_ref[1, group : group + 1, place] = total
            stats_ref[2, group : group + 1, place] = dot


def attention_stats(queries, cots, keys, values, reach, heads, torus):
    blocks, parts = len(queries), len(keys)
    rows = queries[0].shape[0]
    width = heads * REPEAT * HEAD_DIM
    tokens = keys[0].shape[0]
    total = blocks * rows
    saved = shape((heads, parts, tokens, REPEAT * total), jnp.float32)
    held = shape((total, width), jnp.bfloat16)
    outs = [shape((3, heads, REPEAT * total), jnp.float32), saved, saved, held, held]
    return call(
        functools.partial(stats_kernel, torus, blocks, parts),
        outs,
        [VMEM] * (2 * blocks + 3 * parts),
        4 * heads * REPEAT * total * tokens * parts * HEAD_DIM,
    )(*queries, *cots, *keys, *values, *reach)[:4]


def row_scales(group, mine_ref, every_refs):
    at = slice(group, group + 1)
    top = functools.reduce(jnp.maximum, [ref[0, at, :] for ref in every_refs])
    shrink = [jnp.exp(ref[0, at, :] - top) for ref in every_refs]
    total = sum(ref[1, at, :] * factor for ref, factor in zip(every_refs, shrink))
    dot = sum(ref[2, at, :] * factor for ref, factor in zip(every_refs, shrink))
    return jnp.exp(mine_ref[0, at, :] - top) / total, dot / total


def key_gradient(group, stats_refs, expo_ref, grads_ref, query_ref, cosine_ref, sine_ref):
    scale, dot = row_scales(group, stats_refs[0], stats_refs)
    parts, tokens = expo_ref.shape[1:3]
    per, count = chunks(query_ref.shape[0])
    width = per * query_ref.shape[0]
    blocks = []
    for part in range(parts):
        gradient = 0.0
        for chunk in range(count):
            place = slice(chunk * width, (chunk + 1) * width)
            query = heads_of(query_ref, group * REPEAT + chunk * per, per)
            prob = expo_ref[group, part, :, place] * scale[:, place]
            pulled = prob * (grads_ref[group, part, :, place] - dot[:, place])
            gradient += jnp.dot(
                pulled.astype(jnp.bfloat16), query, preferred_element_type=jnp.float32
            )
        gradient = gradient * (HEAD_DIM**-0.5)
        turned = pltpu.roll(gradient, HEAD_DIM // 2, 1)
        at = slice(part * tokens, (part + 1) * tokens)
        blocks.append(
            (gradient * cosine_ref[at, :] + turned * sine_ref[at, :]).astype(jnp.bfloat16)
        )
    return blocks


def grad_kernel(count, *refs):
    stats_refs, out_ref = refs[:count], refs[-1]
    for group in range(stats_refs[0].shape[1]):
        blocks = key_gradient(group, stats_refs, *refs[count:-1])
        out_ref[:, group * HEAD_DIM : (group + 1) * HEAD_DIM] = blocks[0]


def along_z(rows, distance):
    return pl.multiple_of(((position()[3] + distance) & 3) * rows, rows)


def put_product(own_ref, far_ref, unrot_ref, leaves, turns, distances, out_ref):
    first, second = first_second()
    size = out_ref.shape[0] // len(distances)
    quarter = (first ^ leaves) * 2 + (second ^ turns)
    for number, distance in enumerate(distances):
        start = pl.multiple_of(quarter * 4 * size, size) + along_z(size, distance)
        at = pl.ds(pl.multiple_of(start, size), size)
        total = jnp.dot(
            own_ref[at, :], unrot_ref[0], preferred_element_type=jnp.float32
        ) + jnp.dot(far_ref[at, :], unrot_ref[1], preferred_element_type=jnp.float32)
        out_ref[number * size : (number + 1) * size, :] = total.astype(out_ref.dtype)


def send_kernel(chunks_out, *refs):
    stats_refs, saved_refs = refs[:2], refs[2:7]
    own_ref, far_ref, unrot_ref = refs[7:10]
    for group in range(stats_refs[0].shape[1]):
        columns = pl.ds(group * HEAD_DIM, HEAD_DIM)
        for part, block in enumerate(key_gradient(group, stats_refs, *saved_refs)):
            unrot_ref[part, :, columns] = block
    for chunk, out_ref in zip(chunks_out, refs[10:]):
        put_product(own_ref, far_ref, unrot_ref, *chunk, out_ref)


def rest_kernel(chunks_out, own_ref, far_ref, unrot_ref, *outs):
    for chunk, out_ref in zip(chunks_out, outs):
        put_product(own_ref, far_ref, unrot_ref, *chunk, out_ref)


def add_kernel(start, keep_ref, come_ref, out_ref):
    at = pl.ds(start, out_ref.shape[0])
    out_ref[...] = (keep_ref[at, :] + come_ref[...].astype(jnp.float32)).astype(jnp.bfloat16)


def total_kernel(keep_start, stay_start, keep_ref, stay_ref, come_ref, *outs):
    rows = outs[0].shape[0]
    for number, out_ref in enumerate(outs):
        total = keep_ref[pl.ds(keep_start + number * rows, rows), :]
        total += stay_ref[pl.ds(stay_start + number * rows, rows), :].astype(jnp.float32)
        total += come_ref[pl.ds(number * rows, rows), :].astype(jnp.float32)
        out_ref[...] = total.astype(out_ref.dtype)


def last_kernel(*refs):
    terms, (here_ref, there_ref) = refs[:4], refs[4:]
    rows = here_ref.shape[0]
    core = position()[0]
    for owner, out_ref in ((1 - core, there_ref), (core, here_ref)):
        at = pl.ds(pl.multiple_of(owner * rows, rows), rows)
        out_ref[...] = sum(ref[at, :].astype(jnp.float32) for ref in terms)


def next_kernel(scale, here_ref, there_ref, hessian_ref, out_ref):
    width = here_ref.shape[1]
    core = position()[0]
    for owner, ref in ((core, here_ref), (1 - core, there_ref)):
        columns = pl.ds(pl.multiple_of(owner * width, width), width)
        term = ref[...]
        out_ref[:, columns] = decay_rate * hessian_ref[:, columns] + scale * term * term


def turn_kernel(features_ref, out_ref):
    rows = out_ref.shape[0] // 32
    core = position()[0]
    for x in range(2):
        for c in range(2):
            part = features_ref[:, pl.ds((x * 2 + c) * 8 * rows, 8 * rows)].T
            for z in range(4):
                for y in range(2):
                    pair = jnp.where(core == 0, x * 2 + y, y * 2 + x)
                    at = pl.multiple_of((pair * 8 + z * 2 + c) * rows, rows)
                    out_ref[pl.ds(at, rows), :] = part[
                        (z * 2 + y) * rows : (z * 2 + y + 1) * rows
                    ]


def own_kernel(blocks, *refs):
    sources, (turned_ref, cosine_ref, sine_ref, reach_ref), rest = refs[:8], refs[8:12], refs[12:]
    held, sems = rest[:-1], rest[-1]
    copies = [
        pltpu.make_async_copy(source, target, sems.at[number])
        for number, (source, target) in enumerate(zip(sources, held))
    ]
    for copy in copies:
        copy.start()
    for copy in copies:
        copy.wait()
    keys_ref, (picked_ref, features_ref, coarse_ref, fine_ref) = held[0], held[4:]
    tokens, blk = keys_ref.shape[0], lax.axis_index("blk")
    reach_ref[...] = reach_of(picked_ref[...], blk, reach_ref.shape[1], blocks, tokens)
    starts = blk * tokens, (blk ^ 1) * tokens
    fill_rotation(starts, tokens, coarse_ref, fine_ref, cosine_ref, sine_ref)
    turn_kernel(features_ref, turned_ref)


def far_kernel(blocks, tokens, features_ref, picked_ref, turned_ref, reach_ref):
    here = lax.axis_index("blk") ^ 1
    reach_ref[...] = reach_of(picked_ref[...], here, reach_ref.shape[1], blocks, tokens)
    turn_kernel(features_ref, turned_ref)


def reduced_on_torus(normed, picked, queries, key_states, values, cotangent, hessian):
    tokens = key_states.shape[0]
    out_rows = hessian.shape[0]
    heads = KV_HEADS // 2

    first = swapped(queries, "blk", 2), swapped(cotangent, "blk", 2)
    second = swapped(queries, "blk", 1), swapped(cotangent, "blk", 1)
    third = swapped(first[0], "blk", 1), swapped(first[1], "blk", 1)
    far_keys, far_values = swapped(key_states, "blk", 1), swapped(values, "blk", 1)
    far_normed, far_picked = swapped(normed, "blk", 1), swapped(picked, "blk", 1)

    coarse, fine = rotation_rows(np.arange(0, 4 * tokens, 16)), rotation_rows(np.arange(16))
    turned = shape((normed.shape[1], tokens), jnp.bfloat16)
    table = shape((2 * tokens, HEAD_DIM), jnp.float32)
    last = shape((1, REPEAT * 4 * queries.shape[0]), jnp.int32)
    given = [
        pltpu.with_memory_space_constraint(array, pltpu.HBM)
        for array in (key_states, values, queries, cotangent, picked, normed, coarse, fine)
    ]
    own, cosine, sine, reach, *fetched = call(
        functools.partial(own_kernel, 4),
        [turned, table, table, last] + [shape(array.shape, array.dtype) for array in given[:4]],
        [HBM] * 8,
        1 << 28,
        [pltpu.VMEM(array.shape, array.dtype) for array in given[4:]]
        + [pltpu.SemaphoreType.DMA((8,))],
    )(*given)
    key_states, values, *held = fetched
    held = [held, second, first, third]
    far, far_reach = call(
        functools.partial(far_kernel, 4, tokens), [turned, last], [VMEM] * 2, 1 << 28
    )(far_normed, far_picked)

    stats, expo, grads, query = attention_stats(
        [pair[0] for pair in held],
        [pair[1] for pair in held],
        [key_states, far_keys],
        [values, far_values],
        (reach, far_reach),
        heads,
        True,
    )
    other = swapped(stats, "blk", 2)

    half_rows = normed.shape[1] // 2
    work = 2 * half_rows * 2 * tokens * heads * HEAD_DIM
    route = [(i, i ^ (1 if (i // 8) % 2 else 16)) for i in range(32)]
    route_after = [(i, i ^ (16 if (i // 8) % 2 else 1)) for i in range(32)]
    rows, wide = half_rows // 8, heads * HEAD_DIM

    def block(chunk, dtype=jnp.bfloat16):
        return shape((rows * len(chunk), wide), dtype)

    early = [(1, 1, chunk) for chunk in TRAVEL[:EARLY]]
    late = [(1, 1, chunk) for chunk in TRAVEL[EARLY:]] + [(1, 0, chunk) for chunk in STAY]
    unrot, *sends = call(
        functools.partial(send_kernel, early),
        [shape((2, tokens, wide), jnp.bfloat16)] + [block(chunk[2]) for chunk in early],
        [VMEM] * 9,
        work,
    )(stats, other, expo, grads, query, cosine, sine, own, far)
    everywhere = sum(TRAVEL, ())
    late.append((0, 1, everywhere))
    *more, turn_keep = call(
        functools.partial(rest_kernel, late),
        [block(chunk[2]) for chunk in late[:-1]] + [block(everywhere, jnp.float32)],
        [VMEM] * 3,
        work,
    )(own, far, unrot)
    sends += more
    (stay_keep,) = call(
        functools.partial(rest_kernel, [(0, 0, everywhere)]),
        [block(everywhere, jnp.float32)],
        [VMEM] * 3,
        work,
    )(own, far, unrot)
    come = []
    for send in sends:
        come.append(lax.ppermute(send, BOTH, route))
    totals = []
    for number, chunk in enumerate(TRAVEL):
        first = everywhere.index(chunk[0])
        send = call(
            functools.partial(add_kernel, rows * first), block(chunk), [VMEM] * 2, 1 << 20
        )(turn_keep, come[number])
        arrived = lax.ppermute(send, BOTH, route_after)
        outs = [block((0,), jnp.bfloat16 if distance else jnp.float32) for distance in chunk]
        source = next(i for i, other in enumerate(STAY) if chunk[0] in other)
        inside = STAY[source].index(chunk[0])
        totals += call(
            functools.partial(total_kernel, rows * first, rows * inside),
            outs,
            [VMEM] * 3,
            1 << 20,
        )(stay_keep, come[len(TRAVEL) + source], arrived)
    sends, mine = totals[:3], totals[3]
    arrived = []
    for distance, send in zip(everywhere, sends):
        along = [(i, (i + 2 * distance) % 8) for i in range(8)]
        arrived.append(lax.ppermute(send, "fsdp", along))
    columns = shape((out_rows, wide), jnp.float32)
    here, there = call(last_kernel, [columns] * 2, [VMEM] * 4, 1 << 20)(mine, *arrived)
    there = swapped(there, "blk", 1)
    return call(
        functools.partial(next_kernel, (1.0 - decay_rate) / lax.axis_size("fsdp")),
        shape(hessian.shape, jnp.float32),
        [VMEM] * 3,
        1 << 20,
    )(here, there, hessian)


def reduced_anywhere(normed, picked, queries, key_states, values, cotangent):
    rows, tokens = queries.shape[0], key_states.shape[0]
    size, blk = lax.axis_size("blk"), lax.axis_index("blk")
    every_query = lax.all_gather(queries, "blk", axis=0)
    every_cot = lax.all_gather(cotangent, "blk", axis=0)
    order = jnp.arange(size, dtype=jnp.int32)
    ids = order[:, None]
    reach = jnp.where(
        ids == blk, picked, jnp.where(ids > blk, jnp.int32(tokens), jnp.int32(-1))
    ).reshape(1, size * rows)
    reach = jnp.tile(reach, (1, chunks(size * rows)[0]))
    cosine, sine = lax.dynamic_index_in_dim(
        rotation_rows(np.arange(size * tokens)).reshape(2, size, tokens, HEAD_DIM), blk, 1, False
    )
    stats, expo, grads, query = attention_stats(
        [every_query[i] for i in range(size)],
        [every_cot[i] for i in range(size)],
        [key_states],
        [values],
        (reach,),
        KV_HEADS,
        False,
    )
    gathered = lax.all_gather(stats, "blk", axis=0)
    others = [gathered[(blk + i) % size] for i in range(1, size)]
    unrotated = call(
        functools.partial(grad_kernel, size),
        shape((tokens, KV_HEADS * HEAD_DIM), jnp.bfloat16),
        [VMEM] * (size + 5),
        1 << 28,
    )(stats, *others, expo, grads, query, cosine, sine)
    term = lax.dot_general(
        normed, unrotated, (((0,), (0,)), ((), ())), preferred_element_type=jnp.float32
    )
    return lax.psum_scatter(term, BOTH, scatter_dimension=0, tiled=True)


def on_torus(blocks, sequences):
    return blocks == 4 and sequences == 8


def local(normed, picked, queries, key_states, values, cotangent, hessian):
    given = (normed[0], picked, queries[0], key_states[0], values[0], cotangent[0])
    rows, tokens, out_rows = queries.shape[1], key_states.shape[1], hessian.shape[0]
    blocks, sequences = lax.axis_size("blk"), lax.axis_size("fsdp")
    fits = rows & (rows - 1) == 0 and rows <= 16 and tokens % 128 == 0 and out_rows % 16 == 0
    if on_torus(blocks, sequences):
        assert fits
        return reduced_on_torus(*given, hessian)
    summed = reduced_anywhere(*given)
    return decay_rate * hessian + (1.0 - decay_rate) * summed * summed / sequences


def solution(mesh):
    placed = (
        P("fsdp", "blk", None),
        P("fsdp", "blk"),
        P("fsdp", "blk", None),
        P("fsdp", "blk", None),
        P("fsdp", "blk", None),
        P("fsdp", "blk", None),
        P(("blk", "fsdp"), None),
    )
    return jax.shard_map(
        local, mesh=mesh, in_specs=placed, out_specs=P(("blk", "fsdp"), None), check_vma=False
    )
```

```python
import functools

import jax
import jax.numpy as jnp
import numpy as np
from jax import lax
from jax.experimental import pallas as pl
from jax.experimental.pallas import tpu as pltpu
from jax.sharding import PartitionSpec as P


HEADS = 16
KV_HEADS = 4
HEAD_DIM = 128
REPEAT = HEADS // KV_HEADS

decay_rate = 0.99
rope_base = 500000.0
neg_large = -1e30

VMEM = pl.BlockSpec(memory_space=pltpu.VMEM)
HBM = pl.BlockSpec(memory_space=pltpu.HBM)
NT_DIMS = (((1,), (1,)), ((), ()))
BOTH = ("blk", "fsdp")
TRAVEL, STAY, EARLY = ((1, 2), (3, 0)), ((1, 2), (3, 0)), 2


def swapped(block, axis, bits):
    route = [(i, i ^ bits) for i in range(lax.axis_size(axis))]
    return lax.ppermute(block, axis, route)


def call(kernel, out_shape, in_specs, flops, scratch=()):
    return pl.pallas_call(
        kernel,
        out_shape=out_shape,
        in_specs=in_specs,
        out_specs=jax.tree.map(lambda _: VMEM, out_shape),
        scratch_shapes=scratch,
        compiler_params=pltpu.CompilerParams(vmem_limit_bytes=16 << 20),
        cost_estimate=pl.CostEstimate(flops=flops, bytes_accessed=1 << 20, transcendentals=0),
    )


def shape(dims, dtype):
    return jax.ShapeDtypeStruct(dims, dtype)


def rotation_rows(positions):
    half = HEAD_DIM // 2
    frequency = rope_base ** (-2.0 * np.arange(half) / HEAD_DIM)
    angles = positions[:, None] * frequency[None, :]
    cosine, sine = np.cos(angles), np.sin(angles)
    pair = np.concatenate([cosine, cosine], -1), np.concatenate([sine, -sine], -1)
    return jnp.asarray(np.stack(pair).astype(np.float32))


def fill_rotation(starts, tokens, coarse_ref, fine_ref, cosine_ref, sine_ref):
    fine_cos, fine_sin = fine_ref[0], fine_ref[1]
    for part, start in enumerate(starts):
        for step in range(tokens // 16):
            row = pl.ds(start // 16 + step, 1)
            cosine, sine = coarse_ref[0, row, :], coarse_ref[1, row, :]
            at = pl.ds(part * tokens + step * 16, 16)
            cosine_ref[at, :] = cosine * fine_cos - sine * fine_sin
            sine_ref[at, :] = sine * fine_cos + cosine * fine_sin


def position():
    blk, fsdp = lax.axis_index("blk"), lax.axis_index("fsdp")
    return blk & 1, blk >> 1, fsdp & 1, fsdp >> 1


def first_second():
    core, side, y, _ = position()
    return jnp.where(core == 0, side, y), jnp.where(core == 0, y, side)


def chunks(rows):
    per = max(1, min(REPEAT, 256 // rows))
    return per, REPEAT // per


def heads_of(held, first, count):
    parts = [held[:, pl.ds((first + r) * HEAD_DIM, HEAD_DIM)] for r in range(count)]
    return parts[0] if count == 1 else jnp.concatenate(parts, axis=0)


def reach_of(picked, here, width, first_block, blocks, tokens):
    rows = picked.shape[1]
    square = (rows, rows)
    diagonal = lax.broadcasted_iota(jnp.int32, square, 0) == lax.broadcasted_iota(
        jnp.int32, square, 1
    )
    column = jnp.sum(jnp.where(diagonal, picked, 0), axis=1, keepdims=True)
    lane = lax.broadcasted_iota(jnp.int32, (rows, width), 1)
    chosen = lax.broadcasted_iota(jnp.int32, (rows, width), 0) == (lane & (rows - 1))
    own = jnp.sum(jnp.where(chosen, column, 0), axis=0, keepdims=True)
    lane = lax.broadcasted_iota(jnp.int32, (1, width), 1)
    block = first_block + ((lane >> (rows.bit_length() - 1)) & (blocks - 1))
    return jnp.where(block == here, own, jnp.where(block > here, tokens, -1))


def fill_stats(columns, reaches, key_refs, value_refs, held, outs):
    query_held, cot_held = held
    stats, expo_ref, grads_ref = outs
    per, count = chunks(query_held.shape[0])
    width = per * query_held.shape[0]
    for group in range(expo_ref.shape[0]):
        at = pl.ds(pl.multiple_of(columns + group * HEAD_DIM, HEAD_DIM), HEAD_DIM)
        for chunk in range(count):
            first = group * REPEAT + chunk * per
            query = heads_of(query_held, first, per)
            cot = heads_of(cot_held, first, per)
            scores, tops = [], []
            for reach, key_ref in zip(reaches, key_refs):
                score = lax.dot_general(
                    key_ref[:, at], query, NT_DIMS, preferred_element_type=jnp.float32
                ) * (HEAD_DIM**-0.5)
                key_ids = lax.broadcasted_iota(jnp.int32, score.shape, 0)
                score = jnp.where(key_ids <= reach, score, neg_large)
                scores.append(score)
                tops.append(jnp.max(score, axis=0, keepdims=True))
            top = functools.reduce(jnp.maximum, tops)
            place = pl.ds(chunk * width, width)
            total, dot = 0.0, 0.0
            for part, (score, value_ref) in enumerate(zip(scores, value_refs)):
                grads = lax.dot_general(
                    value_ref[:, at], cot, NT_DIMS, preferred_element_type=jnp.float32
                )
                expo = jnp.exp(score - top)
                weights = expo.astype(jnp.bfloat16).astype(jnp.float32)
                total += jnp.sum(expo, axis=0, keepdims=True)
                dot += jnp.sum(weights * grads, axis=0, keepdims=True)
                expo_ref[group, part, :, place] = expo
                grads_ref[group, part, :, place] = grads
            for number, value in enumerate((top, total, dot)):
                stats(number)[group : group + 1, place] = value


def hold_rows(places, query_refs, cot_refs, columns, held):
    for place, query_ref, cot_ref in zip(places, query_refs, cot_refs):
        rows = query_ref.shape[0]
        at = pl.ds(pl.multiple_of(place * rows, rows), rows)
        held[0][at, :] = query_ref[:, columns]
        held[1][at, :] = cot_ref[:, columns]


def any_stats_kernel(blocks, *refs):
    query_refs, cot_refs = refs[:blocks], refs[blocks : 2 * blocks]
    key_ref, value_ref, reach_ref, stats_ref, expo_ref, grads_ref, *held = refs[2 * blocks :]
    hold_rows(range(blocks), query_refs, cot_refs, slice(None), held)
    outs = (lambda number: stats_ref.at[number]), expo_ref, grads_ref
    fill_stats(0, [reach_ref[...]], [key_ref], [value_ref], held, outs)


def chip_stats_kernel(side, *refs):
    query_refs, cot_refs, key_refs, value_refs = (refs[2 * i : 2 * i + 2] for i in range(4))
    rest, (stats_ref, expo_ref, grads_ref, *held) = refs[8:-5], refs[-5:]
    blk = lax.axis_index("blk")
    core, chip = blk & 1, blk >> 1
    tokens, width = key_refs[0].shape[0], held[0].shape[1]
    if side == 0:
        lanes = expo_ref.shape[3]
        reaches = [
            reach_of(ref[...], blk ^ part, lanes, chip * 2, 2, tokens)
            for part, ref in enumerate(rest)
        ]
        outs = lambda number: stats_ref.at[number]
    else:
        reaches = [jnp.where(chip == 0, tokens, -1)] * 2
        stats_ref[:, 0] = rest[0][...]
        outs = lambda number: stats_ref.at[number, 1]
    start = core * width
    columns = pl.ds(pl.multiple_of(start, HEAD_DIM), width)
    hold_rows((core, 1 - core), query_refs, cot_refs, columns, held)
    heads = core * (HEAD_DIM * expo_ref.shape[0])
    fill_stats(heads, reaches, key_refs, value_refs, held, (outs, expo_ref, grads_ref))


def attention_stats(kernel, queries, cots, keys, values, more, heads, sides=()):
    parts, (rows, tokens) = len(keys), (queries[0].shape[0], keys[0].shape[0])
    total, width = len(queries) * rows, heads * REPEAT * HEAD_DIM
    saved = shape((heads, parts, tokens, REPEAT * total), jnp.float32)
    held = shape((total, width), jnp.bfloat16)
    outs = [shape((3, *sides, heads, REPEAT * total), jnp.float32), saved, saved, held, held]
    operands = (*queries, *cots, *keys, *values, *more)
    flops = 4 * heads * REPEAT * total * tokens * parts * HEAD_DIM
    return call(kernel, outs, [VMEM] * len(operands), flops)(*operands)[:4]


def row_scales(every):
    tops, totals, dots = zip(*every)
    top = functools.reduce(jnp.maximum, tops)
    shrink = [jnp.exp(value - top) for value in tops]
    total = sum(value * factor for value, factor in zip(totals, shrink))
    dot = sum(value * factor for value, factor in zip(dots, shrink))
    return shrink[0] / total, dot / total


def key_gradient(group, sets, cosine_ref, sine_ref):
    scales = [row_scales(rows[0]) for rows in sets]
    parts, tokens = sets[0][1].shape[1:3]
    per, count = chunks(sets[0][3].shape[0])
    width = per * sets[0][3].shape[0]
    blocks = []
    for part in range(parts):
        gradient = 0.0
        for chunk in range(count):
            place = slice(chunk * width, (chunk + 1) * width)
            pulled, queries = [], []
            for (scale, dot), (_, expo_ref, grads_ref, query_ref) in zip(scales, sets):
                queries.append(heads_of(query_ref, group * REPEAT + chunk * per, per))
                prob = expo_ref[group, part, :, place] * scale[:, place]
                grads = prob * (grads_ref[group, part, :, place] - dot[:, place])
                pulled.append(grads.astype(jnp.bfloat16))
            gradient += jnp.dot(
                pulled[0] if len(sets) == 1 else jnp.concatenate(pulled, axis=1),
                queries[0] if len(sets) == 1 else jnp.concatenate(queries, axis=0),
                preferred_element_type=jnp.float32,
            )
        gradient = gradient * (HEAD_DIM**-0.5)
        turned = pltpu.roll(gradient, HEAD_DIM // 2, 1)
        at = slice(part * tokens, (part + 1) * tokens)
        blocks.append(
            (gradient * cosine_ref[at, :] + turned * sine_ref[at, :]).astype(jnp.bfloat16)
        )
    return blocks


def grad_kernel(count, *refs):
    expo_ref, grads_ref, query_ref, cosine_ref, sine_ref, out_ref = refs[count:]
    for group in range(expo_ref.shape[0]):
        at = slice(group, group + 1)
        every = [[ref[number, at, :] for number in range(3)] for ref in refs[:count]]
        sets = [(every, expo_ref, grads_ref, query_ref)]
        blocks = key_gradient(group, sets, cosine_ref, sine_ref)
        out_ref[:, group * HEAD_DIM : (group + 1) * HEAD_DIM] = blocks[0]


def along_z(rows, distance):
    return pl.multiple_of(((position()[3] + distance) & 3) * rows, rows)


def put_product(own_ref, far_ref, unrot_ref, leaves, turns, distances, out_ref):
    first, second = first_second()
    size = out_ref.shape[0] // len(distances)
    quarter = (first ^ leaves) * 2 + (second ^ turns)
    for number, distance in enumerate(distances):
        start = pl.multiple_of(quarter * 4 * size, size) + along_z(size, distance)
        at = pl.ds(pl.multiple_of(start, size), size)
        total = jnp.dot(
            own_ref[at, :], unrot_ref[0], preferred_element_type=jnp.float32
        ) + jnp.dot(far_ref[at, :], unrot_ref[1], preferred_element_type=jnp.float32)
        out_ref[number * size : (number + 1) * size, :] = total.astype(out_ref.dtype)


def send_kernel(chunks_out, mine_ref, other_ref, *refs):
    saved_refs, tables, (own_ref, far_ref, unrot_ref) = refs[:6], refs[6:8], refs[8:11]
    for group in range(saved_refs[0].shape[0]):
        at = slice(group, group + 1)
        sets = []
        for side in range(2):
            mine = [mine_ref[number, side, at, :] for number in range(3)]
            other = [other_ref[number, 1 - side, at, :] for number in range(3)]
            sets.append(((mine, other), *saved_refs[3 * side : 3 * side + 3]))
        columns = pl.ds(group * HEAD_DIM, HEAD_DIM)
        for part, block in enumerate(key_gradient(group, sets, *tables)):
            unrot_ref[part, :, columns] = block
    for chunk, out_ref in zip(chunks_out, refs[11:]):
        put_product(own_ref, far_ref, unrot_ref, *chunk, out_ref)


def rest_kernel(chunks_out, own_ref, far_ref, unrot_ref, *outs):
    for chunk, out_ref in zip(chunks_out, outs):
        put_product(own_ref, far_ref, unrot_ref, *chunk, out_ref)


def add_kernel(start, keep_ref, come_ref, out_ref):
    at = pl.ds(start, out_ref.shape[0])
    out_ref[...] = (keep_ref[at, :] + come_ref[...].astype(jnp.float32)).astype(jnp.bfloat16)


def total_kernel(keep_start, stay_start, keep_ref, stay_ref, come_ref, *outs):
    rows = outs[0].shape[0]
    for number, out_ref in enumerate(outs):
        total = keep_ref[pl.ds(keep_start + number * rows, rows), :]
        total += stay_ref[pl.ds(stay_start + number * rows, rows), :].astype(jnp.float32)
        total += come_ref[pl.ds(number * rows, rows), :].astype(jnp.float32)
        out_ref[...] = total.astype(out_ref.dtype)


def last_kernel(*refs):
    terms, (here_ref, there_ref) = refs[:4], refs[4:]
    rows = here_ref.shape[0]
    core = position()[0]
    for owner, out_ref in ((1 - core, there_ref), (core, here_ref)):
        at = pl.ds(pl.multiple_of(owner * rows, rows), rows)
        out_ref[...] = sum(ref[at, :].astype(jnp.float32) for ref in terms)


def next_kernel(scale, here_ref, there_ref, hessian_ref, out_ref):
    width = here_ref.shape[1]
    core = position()[0]
    for owner, ref in ((core, here_ref), (1 - core, there_ref)):
        columns = pl.ds(pl.multiple_of(owner * width, width), width)
        term = ref[...]
        out_ref[:, columns] = decay_rate * hessian_ref[:, columns] + scale * term * term


def turn_kernel(features_ref, out_ref):
    rows = out_ref.shape[0] // 32
    core = position()[0]
    for x in range(2):
        for c in range(2):
            part = features_ref[:, pl.ds((x * 2 + c) * 8 * rows, 8 * rows)].T
            for z in range(4):
                for y in range(2):
                    pair = jnp.where(core == 0, x * 2 + y, y * 2 + x)
                    at = pl.multiple_of((pair * 8 + z * 2 + c) * rows, rows)
                    out_ref[pl.ds(at, rows), :] = part[
                        (z * 2 + y) * rows : (z * 2 + y + 1) * rows
                    ]


def own_kernel(*refs):
    sources, (turned_ref, cosine_ref, sine_ref), rest = refs[:8], refs[8:11], refs[11:]
    held, sems = rest[:-1], rest[-1]
    copies = [
        pltpu.make_async_copy(source, target, sems.at[number])
        for number, (source, target) in enumerate(zip(sources, held))
    ]
    for copy in copies:
        copy.start()
    for copy in copies:
        copy.wait()
    features_ref, coarse_ref, fine_ref = held[5:]
    tokens, blk = held[0].shape[0], lax.axis_index("blk")
    starts = blk * tokens, (blk ^ 1) * tokens
    fill_rotation(starts, tokens, coarse_ref, fine_ref, cosine_ref, sine_ref)
    turn_kernel(features_ref, turned_ref)


def reduced_on_torus(normed, picked, queries, key_states, values, cotangent, hessian):
    tokens = key_states.shape[0]
    out_rows = hessian.shape[0]
    heads = KV_HEADS // 2

    first = swapped(queries, "blk", 2), swapped(cotangent, "blk", 2)
    second = swapped(queries, "blk", 1), swapped(cotangent, "blk", 1)
    third = swapped(first[0], "blk", 1), swapped(first[1], "blk", 1)
    far_keys, far_values = swapped(key_states, "blk", 1), swapped(values, "blk", 1)
    far_normed, far_picked = swapped(normed, "blk", 1), swapped(picked, "blk", 1)

    coarse, fine = rotation_rows(np.arange(0, 4 * tokens, 16)), rotation_rows(np.arange(16))
    turned = shape((normed.shape[1], tokens), jnp.bfloat16)
    table = shape((2 * tokens, HEAD_DIM), jnp.float32)
    given = [
        pltpu.with_memory_space_constraint(array, pltpu.HBM)
        for array in (key_states, values, queries, cotangent, picked, normed, coarse, fine)
    ]
    own, cosine, sine, key_states, values, queries, cotangent, picked = call(
        own_kernel,
        [turned, table, table] + [shape(array.shape, array.dtype) for array in given[:5]],
        [HBM] * 8,
        1 << 28,
        [pltpu.VMEM(array.shape, array.dtype) for array in given[5:]]
        + [pltpu.SemaphoreType.DMA((8,))],
    )(*given)
    far = call(turn_kernel, turned, [VMEM], 1 << 28)(far_normed)

    keys, values = [key_states, far_keys], [values, far_values]
    stats, *near = attention_stats(
        functools.partial(chip_stats_kernel, 0),
        (queries, second[0]),
        (cotangent, second[1]),
        keys,
        values,
        (picked, far_picked),
        heads,
    )
    stats, *across = attention_stats(
        functools.partial(chip_stats_kernel, 1),
        (first[0], third[0]),
        (first[1], third[1]),
        keys,
        values,
        (stats,),
        heads,
        (2,),
    )
    other = swapped(stats, "blk", 2)

    half_rows = normed.shape[1] // 2
    work = 2 * half_rows * 2 * tokens * heads * HEAD_DIM
    route = [(i, i ^ (1 if (i // 8) % 2 else 16)) for i in range(32)]
    route_after = [(i, i ^ (16 if (i // 8) % 2 else 1)) for i in range(32)]
    rows, wide = half_rows // 8, heads * HEAD_DIM

    def block(chunk, dtype=jnp.bfloat16):
        return shape((rows * len(chunk), wide), dtype)

    early = [(1, 1, chunk) for chunk in TRAVEL[:EARLY]]
    late = [(1, 1, chunk) for chunk in TRAVEL[EARLY:]] + [(1, 0, chunk) for chunk in STAY]
    unrot, *sends = call(
        functools.partial(send_kernel, early),
        [shape((2, tokens, wide), jnp.bfloat16)] + [block(chunk[2]) for chunk in early],
        [VMEM] * 12,
        work,
    )(stats, other, *near, *across, cosine, sine, own, far)
    everywhere = sum(TRAVEL, ())
    late.append((0, 1, everywhere))
    *more, turn_keep = call(
        functools.partial(rest_kernel, late),
        [block(chunk[2]) for chunk in late[:-1]] + [block(everywhere, jnp.float32)],
        [VMEM] * 3,
        work,
    )(own, far, unrot)
    sends += more
    (stay_keep,) = call(
        functools.partial(rest_kernel, [(0, 0, everywhere)]),
        [block(everywhere, jnp.float32)],
        [VMEM] * 3,
        work,
    )(own, far, unrot)
    come = []
    for send in sends:
        come.append(lax.ppermute(send, BOTH, route))
    totals = []
    for number, chunk in enumerate(TRAVEL):
        first = everywhere.index(chunk[0])
        send = call(
            functools.partial(add_kernel, rows * first), block(chunk), [VMEM] * 2, 1 << 20
        )(turn_keep, come[number])
        arrived = lax.ppermute(send, BOTH, route_after)
        outs = [block((0,), jnp.bfloat16 if distance else jnp.float32) for distance in chunk]
        source = next(i for i, other in enumerate(STAY) if chunk[0] in other)
        inside = STAY[source].index(chunk[0])
        totals += call(
            functools.partial(total_kernel, rows * first, rows * inside),
            outs,
            [VMEM] * 3,
            1 << 20,
        )(stay_keep, come[len(TRAVEL) + source], arrived)
    sends, mine = totals[:3], totals[3]
    arrived = []
    for distance, send in zip(everywhere, sends):
        along = [(i, (i + 2 * distance) % 8) for i in range(8)]
        arrived.append(lax.ppermute(send, "fsdp", along))
    columns = shape((out_rows, wide), jnp.float32)
    here, there = call(last_kernel, [columns] * 2, [VMEM] * 4, 1 << 20)(mine, *arrived)
    there = swapped(there, "blk", 1)
    return call(
        functools.partial(next_kernel, (1.0 - decay_rate) / lax.axis_size("fsdp")),
        shape(hessian.shape, jnp.float32),
        [VMEM] * 3,
        1 << 20,
    )(here, there, hessian)


def reduced_anywhere(normed, picked, queries, key_states, values, cotangent):
    rows, tokens = queries.shape[0], key_states.shape[0]
    size, blk = lax.axis_size("blk"), lax.axis_index("blk")
    every_query = lax.all_gather(queries, "blk", axis=0)
    every_cot = lax.all_gather(cotangent, "blk", axis=0)
    order = jnp.arange(size, dtype=jnp.int32)
    ids = order[:, None]
    reach = jnp.where(
        ids == blk, picked, jnp.where(ids > blk, jnp.int32(tokens), jnp.int32(-1))
    ).reshape(1, size * rows)
    reach = jnp.tile(reach, (1, chunks(size * rows)[0]))
    cosine, sine = lax.dynamic_index_in_dim(
        rotation_rows(np.arange(size * tokens)).reshape(2, size, tokens, HEAD_DIM), blk, 1, False
    )
    stats, expo, grads, query = attention_stats(
        functools.partial(any_stats_kernel, size),
        [every_query[i] for i in range(size)],
        [every_cot[i] for i in range(size)],
        [key_states],
        [values],
        (reach,),
        KV_HEADS,
    )
    gathered = lax.all_gather(stats, "blk", axis=0)
    others = [gathered[(blk + i) % size] for i in range(1, size)]
    unrotated = call(
        functools.partial(grad_kernel, size),
        shape((tokens, KV_HEADS * HEAD_DIM), jnp.bfloat16),
        [VMEM] * (size + 5),
        1 << 28,
    )(stats, *others, expo, grads, query, cosine, sine)
    term = lax.dot_general(
        normed, unrotated, (((0,), (0,)), ((), ())), preferred_element_type=jnp.float32
    )
    return lax.psum_scatter(term, BOTH, scatter_dimension=0, tiled=True)


def on_torus(blocks, sequences):
    return blocks == 4 and sequences == 8


def local(normed, picked, queries, key_states, values, cotangent, hessian):
    given = (normed[0], picked, queries[0], key_states[0], values[0], cotangent[0])
    rows, tokens, out_rows = queries.shape[1], key_states.shape[1], hessian.shape[0]
    blocks, sequences = lax.axis_size("blk"), lax.axis_size("fsdp")
    fits = rows & (rows - 1) == 0 and rows <= 16 and tokens % 128 == 0 and out_rows % 16 == 0
    if on_torus(blocks, sequences):
        assert fits
        return reduced_on_torus(*given, hessian)
    summed = reduced_anywhere(*given)
    return decay_rate * hessian + (1.0 - decay_rate) * summed * summed / sequences


def solution(mesh):
    placed = (
        P("fsdp", "blk", None),
        P("fsdp", "blk"),
        P("fsdp", "blk", None),
        P("fsdp", "blk", None),
        P("fsdp", "blk", None),
        P("fsdp", "blk", None),
        P(("blk", "fsdp"), None),
    )
    return jax.shard_map(
        local, mesh=mesh, in_specs=placed, out_specs=P(("blk", "fsdp"), None), check_vma=False
    )
```

```python
import functools

import jax
import jax.numpy as jnp
import numpy as np
from jax import lax
from jax.experimental import pallas as pl
from jax.experimental.pallas import tpu as pltpu
from jax.sharding import PartitionSpec as P


HEADS = 16
KV_HEADS = 4
HEAD_DIM = 128
REPEAT = HEADS // KV_HEADS

decay_rate = 0.99
rope_base = 500000.0
neg_large = -1e30

VMEM = pl.BlockSpec(memory_space=pltpu.VMEM)
HBM = pl.BlockSpec(memory_space=pltpu.HBM)
NT_DIMS = (((1,), (1,)), ((), ()))
BOTH = ("blk", "fsdp")
TRAVEL, STAY, EARLY = ((1, 2), (3, 0)), ((1, 2), (3, 0)), 2


def swapped(block, axis, bits):
    route = [(i, i ^ bits) for i in range(lax.axis_size(axis))]
    return lax.ppermute(block, axis, route)


def call(kernel, out_shape, in_specs, flops, scratch=()):
    return pl.pallas_call(
        kernel,
        out_shape=out_shape,
        in_specs=in_specs,
        out_specs=jax.tree.map(lambda _: VMEM, out_shape),
        scratch_shapes=scratch,
        compiler_params=pltpu.CompilerParams(vmem_limit_bytes=16 << 20),
        cost_estimate=pl.CostEstimate(flops=flops, bytes_accessed=1 << 20, transcendentals=0),
    )


def shape(dims, dtype):
    return jax.ShapeDtypeStruct(dims, dtype)


def rotation_rows(positions):
    half = HEAD_DIM // 2
    frequency = rope_base ** (-2.0 * np.arange(half) / HEAD_DIM)
    angles = positions[:, None] * frequency[None, :]
    cosine, sine = np.cos(angles), np.sin(angles)
    pair = np.concatenate([cosine, cosine], -1), np.concatenate([sine, -sine], -1)
    return jnp.asarray(np.stack(pair).astype(np.float32))


def fill_rotation(starts, tokens, coarse_ref, fine_ref, cosine_ref, sine_ref):
    fine_cos, fine_sin = fine_ref[0], fine_ref[1]
    for part, start in enumerate(starts):
        for step in range(tokens // 16):
            row = pl.ds(start // 16 + step, 1)
            cosine, sine = coarse_ref[0, row, :], coarse_ref[1, row, :]
            at = pl.ds(part * tokens + step * 16, 16)
            cosine_ref[at, :] = cosine * fine_cos - sine * fine_sin
            sine_ref[at, :] = sine * fine_cos + cosine * fine_sin


def position():
    blk, fsdp = lax.axis_index("blk"), lax.axis_index("fsdp")
    return blk & 1, blk >> 1, fsdp & 1, fsdp >> 1


def first_second():
    core, side, y, _ = position()
    return jnp.where(core == 0, side, y), jnp.where(core == 0, y, side)


def chunks(rows):
    per = max(1, min(REPEAT, 256 // rows))
    return per, REPEAT // per


def heads_of(held, first, count):
    parts = [held[:, pl.ds((first + r) * HEAD_DIM, HEAD_DIM)] for r in range(count)]
    return parts[0] if count == 1 else jnp.concatenate(parts, axis=0)


def reach_of(picked, here, width, first_block, blocks, tokens):
    rows = picked.shape[1]
    square = (rows, rows)
    diagonal = lax.broadcasted_iota(jnp.int32, square, 0) == lax.broadcasted_iota(
        jnp.int32, square, 1
    )
    column = jnp.sum(jnp.where(diagonal, picked, 0), axis=1, keepdims=True)
    lane = lax.broadcasted_iota(jnp.int32, (rows, width), 1)
    chosen = lax.broadcasted_iota(jnp.int32, (rows, width), 0) == (lane & (rows - 1))
    own = jnp.sum(jnp.where(chosen, column, 0), axis=0, keepdims=True)
    lane = lax.broadcasted_iota(jnp.int32, (1, width), 1)
    block = first_block + ((lane >> (rows.bit_length() - 1)) & (blocks - 1))
    return jnp.where(block == here, own, jnp.where(block > here, tokens, -1))


def fill_stats(columns, reaches, key_refs, value_refs, held, outs):
    query_held, cot_held = held
    stats, expo_ref, grads_ref = outs
    per, count = chunks(query_held.shape[0])
    width = per * query_held.shape[0]
    for group in range(expo_ref.shape[0]):
        at = pl.ds(pl.multiple_of(columns + group * HEAD_DIM, HEAD_DIM), HEAD_DIM)
        for chunk in range(count):
            first = group * REPEAT + chunk * per
            query = heads_of(query_held, first, per)
            cot = heads_of(cot_held, first, per)
            scores, tops = [], []
            for reach, key_ref in zip(reaches, key_refs):
                score = lax.dot_general(
                    key_ref[:, at], query, NT_DIMS, preferred_element_type=jnp.float32
                ) * (HEAD_DIM**-0.5)
                key_ids = lax.broadcasted_iota(jnp.int32, score.shape, 0)
                score = jnp.where(key_ids <= reach, score, neg_large)
                scores.append(score)
                tops.append(jnp.max(score, axis=0, keepdims=True))
            top = functools.reduce(jnp.maximum, tops)
            place = pl.ds(chunk * width, width)
            total, dot = 0.0, 0.0
            for part, (score, value_ref) in enumerate(zip(scores, value_refs)):
                grads = lax.dot_general(
                    value_ref[:, at], cot, NT_DIMS, preferred_element_type=jnp.float32
                )
                expo = jnp.exp(score - top)
                weights = expo.astype(jnp.bfloat16).astype(jnp.float32)
                total += jnp.sum(expo, axis=0, keepdims=True)
                dot += jnp.sum(weights * grads, axis=0, keepdims=True)
                expo_ref[group, part, :, place] = expo
                grads_ref[group, part, :, place] = grads
            for number, value in enumerate((top, total, dot)):
                stats(number)[group : group + 1, place] = value


def hold_rows(places, query_refs, cot_refs, columns, held):
    for place, query_ref, cot_ref in zip(places, query_refs, cot_refs):
        rows = query_ref.shape[0]
        at = pl.ds(pl.multiple_of(place * rows, rows), rows)
        held[0][at, :] = query_ref[:, columns]
        held[1][at, :] = cot_ref[:, columns]


def any_stats_kernel(blocks, *refs):
    query_refs, cot_refs = refs[:blocks], refs[blocks : 2 * blocks]
    key_ref, value_ref, reach_ref, stats_ref, expo_ref, grads_ref, *held = refs[2 * blocks :]
    hold_rows(range(blocks), query_refs, cot_refs, slice(None), held)
    outs = (lambda number: stats_ref.at[number]), expo_ref, grads_ref
    fill_stats(0, [reach_ref[...]], [key_ref], [value_ref], held, outs)


def chip_stats_kernel(side, *refs):
    query_refs, cot_refs, key_refs, value_refs = (refs[2 * i : 2 * i + 2] for i in range(4))
    rest, (stats_ref, expo_ref, grads_ref, *held) = refs[8:-5], refs[-5:]
    blk = lax.axis_index("blk")
    core, chip = blk & 1, blk >> 1
    tokens, width = key_refs[0].shape[0], held[0].shape[1]
    if side == 0:
        lanes = expo_ref.shape[3]
        reaches = [
            reach_of(ref[...], blk ^ part, lanes, chip * 2, 2, tokens)
            for part, ref in enumerate(rest)
        ]
        outs = lambda number: stats_ref.at[number]
    else:
        reaches = [jnp.where(chip == 0, tokens, -1)] * 2
        stats_ref[:, 0] = rest[0][...]
        outs = lambda number: stats_ref.at[number, 1]
    start = core * width
    columns = pl.ds(pl.multiple_of(start, HEAD_DIM), width)
    hold_rows((core, 1 - core), query_refs, cot_refs, columns, held)
    heads = core * (HEAD_DIM * expo_ref.shape[0])
    fill_stats(heads, reaches, key_refs, value_refs, held, (outs, expo_ref, grads_ref))


def attention_stats(kernel, queries, cots, keys, values, more, heads, sides=()):
    parts, (rows, tokens) = len(keys), (queries[0].shape[0], keys[0].shape[0])
    total, width = len(queries) * rows, heads * REPEAT * HEAD_DIM
    saved = shape((heads, parts, tokens, REPEAT * total), jnp.float32)
    held = shape((total, width), jnp.bfloat16)
    outs = [shape((3, *sides, heads, REPEAT * total), jnp.float32), saved, saved, held, held]
    operands = (*queries, *cots, *keys, *values, *more)
    flops = 4 * heads * REPEAT * total * tokens * parts * HEAD_DIM
    return call(kernel, outs, [VMEM] * len(operands), flops)(*operands)[:4]


def row_scales(every):
    tops, totals, dots = zip(*every)
    top = functools.reduce(jnp.maximum, tops)
    shrink = [jnp.exp(value - top) for value in tops]
    total = sum(value * factor for value, factor in zip(totals, shrink))
    dot = sum(value * factor for value, factor in zip(dots, shrink))
    return shrink[0] / total, dot / total


def key_gradient(group, sets, cosine_ref, sine_ref):
    scales = [row_scales(rows[0]) for rows in sets]
    parts, tokens = sets[0][1].shape[1:3]
    per, count = chunks(sets[0][3].shape[0])
    width = per * sets[0][3].shape[0]
    blocks = []
    for part in range(parts):
        gradient = 0.0
        for chunk in range(count):
            place = slice(chunk * width, (chunk + 1) * width)
            pulled, queries = [], []
            for (scale, dot), (_, expo_ref, grads_ref, query_ref) in zip(scales, sets):
                queries.append(heads_of(query_ref, group * REPEAT + chunk * per, per))
                prob = expo_ref[group, part, :, place] * scale[:, place]
                grads = prob * (grads_ref[group, part, :, place] - dot[:, place])
                pulled.append(grads.astype(jnp.bfloat16))
            gradient += jnp.dot(
                pulled[0] if len(sets) == 1 else jnp.concatenate(pulled, axis=1),
                queries[0] if len(sets) == 1 else jnp.concatenate(queries, axis=0),
                preferred_element_type=jnp.float32,
            )
        gradient = gradient * (HEAD_DIM**-0.5)
        turned = pltpu.roll(gradient, HEAD_DIM // 2, 1)
        at = slice(part * tokens, (part + 1) * tokens)
        blocks.append(
            (gradient * cosine_ref[at, :] + turned * sine_ref[at, :]).astype(jnp.bfloat16)
        )
    return blocks


def grad_kernel(count, *refs):
    expo_ref, grads_ref, query_ref, cosine_ref, sine_ref, out_ref = refs[count:]
    for group in range(expo_ref.shape[0]):
        at = slice(group, group + 1)
        every = [[ref[number, at, :] for number in range(3)] for ref in refs[:count]]
        sets = [(every, expo_ref, grads_ref, query_ref)]
        blocks = key_gradient(group, sets, cosine_ref, sine_ref)
        out_ref[:, group * HEAD_DIM : (group + 1) * HEAD_DIM] = blocks[0]


def along_z(rows, distance):
    return pl.multiple_of(((position()[3] + distance) & 3) * rows, rows)


def put_product(own_ref, far_ref, unrot_ref, leaves, turns, distances, out_ref):
    first, second = first_second()
    size = out_ref.shape[0] // len(distances)
    quarter = (first ^ leaves) * 2 + (second ^ turns)
    for number, distance in enumerate(distances):
        start = pl.multiple_of(quarter * 4 * size, size) + along_z(size, distance)
        at = pl.ds(pl.multiple_of(start, size), size)
        total = jnp.dot(
            own_ref[at, :], unrot_ref[0], preferred_element_type=jnp.float32
        ) + jnp.dot(far_ref[at, :], unrot_ref[1], preferred_element_type=jnp.float32)
        out_ref[number * size : (number + 1) * size, :] = total.astype(out_ref.dtype)


def send_kernel(chunks_out, mine_ref, other_ref, *refs):
    saved_refs, tables, (own_ref, far_ref, unrot_ref) = refs[:6], refs[6:8], refs[8:11]
    for group in range(saved_refs[0].shape[0]):
        at = slice(group, group + 1)
        sets = []
        for side in range(2):
            mine = [mine_ref[number, side, at, :] for number in range(3)]
            other = [other_ref[number, 1 - side, at, :] for number in range(3)]
            sets.append(((mine, other), *saved_refs[3 * side : 3 * side + 3]))
        columns = pl.ds(group * HEAD_DIM, HEAD_DIM)
        for part, block in enumerate(key_gradient(group, sets, *tables)):
            unrot_ref[part, :, columns] = block
    for chunk, out_ref in zip(chunks_out, refs[11:]):
        put_product(own_ref, far_ref, unrot_ref, *chunk, out_ref)


def rest_kernel(chunks_out, own_ref, far_ref, unrot_ref, *outs):
    for chunk, out_ref in zip(chunks_out, outs):
        put_product(own_ref, far_ref, unrot_ref, *chunk, out_ref)


def add_kernel(start, keep_ref, come_ref, out_ref):
    at = pl.ds(start, out_ref.shape[0])
    out_ref[...] = (keep_ref[at, :] + come_ref[...].astype(jnp.float32)).astype(jnp.bfloat16)


def total_kernel(keep_start, stay_start, keep_ref, stay_ref, come_ref, *outs):
    rows = outs[0].shape[0]
    for number, out_ref in enumerate(outs):
        total = keep_ref[pl.ds(keep_start + number * rows, rows), :]
        total += stay_ref[pl.ds(stay_start + number * rows, rows), :].astype(jnp.float32)
        total += come_ref[pl.ds(number * rows, rows), :].astype(jnp.float32)
        out_ref[...] = total.astype(out_ref.dtype)


def last_total_kernel(
    keep_start, stay_start, keep_ref, stay_ref, come_ref, same_ref, cross_ref, mine_ref
):
    half = same_ref.shape[0]
    core = position()[0]
    for start, size, out_ref in (
        (core * half, half, same_ref),
        ((1 - core) * half, half, cross_ref),
        (2 * half, 2 * half, mine_ref),
    ):
        total = keep_ref[pl.ds(pl.multiple_of(keep_start + start, half), size), :]
        for first, ref in ((stay_start, stay_ref), (0, come_ref)):
            at = pl.ds(pl.multiple_of(first + start, half), size)
            total += ref[at, :].astype(jnp.float32)
        out_ref[...] = total.astype(out_ref.dtype)


def last_kernel(*refs):
    terms, (here_ref, there_ref) = refs[:-2], refs[-2:]
    rows = here_ref.shape[0]
    core = position()[0]
    for owner, out_ref in ((1 - core, there_ref), (core, here_ref)):
        at = pl.ds(pl.multiple_of(owner * rows, rows), rows)
        out_ref[...] = sum(ref[at, :].astype(jnp.float32) for ref in terms)


def next_kernel(scale, here_ref, same_ref, there_ref, cross_ref, hessian_ref, out_ref):
    width = here_ref.shape[1]
    core = position()[0]
    for owner, near, far in ((core, here_ref, same_ref), (1 - core, there_ref, cross_ref)):
        columns = pl.ds(pl.multiple_of(owner * width, width), width)
        term = near[...] + far[...].astype(jnp.float32)
        out_ref[:, columns] = decay_rate * hessian_ref[:, columns] + scale * term * term


def turn_kernel(features_ref, out_ref):
    rows = out_ref.shape[0] // 32
    core = position()[0]
    for x in range(2):
        for c in range(2):
            part = features_ref[:, pl.ds((x * 2 + c) * 8 * rows, 8 * rows)].T
            for z in range(4):
                for y in range(2):
                    pair = jnp.where(core == 0, x * 2 + y, y * 2 + x)
                    at = pl.multiple_of((pair * 8 + z * 2 + c) * rows, rows)
                    out_ref[pl.ds(at, rows), :] = part[
                        (z * 2 + y) * rows : (z * 2 + y + 1) * rows
                    ]


def own_kernel(*refs):
    sources, (turned_ref, cosine_ref, sine_ref), rest = refs[:8], refs[8:11], refs[11:]
    held, sems = rest[:-1], rest[-1]
    copies = [
        pltpu.make_async_copy(source, target, sems.at[number])
        for number, (source, target) in enumerate(zip(sources, held))
    ]
    for copy in copies:
        copy.start()
    for copy in copies:
        copy.wait()
    features_ref, coarse_ref, fine_ref = held[5:]
    tokens, blk = held[0].shape[0], lax.axis_index("blk")
    starts = blk * tokens, (blk ^ 1) * tokens
    fill_rotation(starts, tokens, coarse_ref, fine_ref, cosine_ref, sine_ref)
    turn_kernel(features_ref, turned_ref)


def reduced_on_torus(normed, picked, queries, key_states, values, cotangent, hessian):
    tokens = key_states.shape[0]
    out_rows = hessian.shape[0]
    heads = KV_HEADS // 2

    first = swapped(queries, "blk", 2), swapped(cotangent, "blk", 2)
    second = swapped(queries, "blk", 1), swapped(cotangent, "blk", 1)
    third = swapped(first[0], "blk", 1), swapped(first[1], "blk", 1)
    far_keys, far_values = swapped(key_states, "blk", 1), swapped(values, "blk", 1)
    far_normed, far_picked = swapped(normed, "blk", 1), swapped(picked, "blk", 1)

    coarse, fine = rotation_rows(np.arange(0, 4 * tokens, 16)), rotation_rows(np.arange(16))
    turned = shape((normed.shape[1], tokens), jnp.bfloat16)
    table = shape((2 * tokens, HEAD_DIM), jnp.float32)
    given = [
        pltpu.with_memory_space_constraint(array, pltpu.HBM)
        for array in (key_states, values, queries, cotangent, picked, normed, coarse, fine)
    ]
    own, cosine, sine, key_states, values, queries, cotangent, picked = call(
        own_kernel,
        [turned, table, table] + [shape(array.shape, array.dtype) for array in given[:5]],
        [HBM] * 8,
        1 << 28,
        [pltpu.VMEM(array.shape, array.dtype) for array in given[5:]]
        + [pltpu.SemaphoreType.DMA((8,))],
    )(*given)
    far = call(turn_kernel, turned, [VMEM], 1 << 28)(far_normed)

    keys, values = [key_states, far_keys], [values, far_values]
    stats, *near = attention_stats(
        functools.partial(chip_stats_kernel, 0),
        (queries, second[0]),
        (cotangent, second[1]),
        keys,
        values,
        (picked, far_picked),
        heads,
    )
    stats, *across = attention_stats(
        functools.partial(chip_stats_kernel, 1),
        (first[0], third[0]),
        (first[1], third[1]),
        keys,
        values,
        (stats,),
        heads,
        (2,),
    )
    other = swapped(stats, "blk", 2)

    half_rows = normed.shape[1] // 2
    work = 2 * half_rows * 2 * tokens * heads * HEAD_DIM
    route = [(i, i ^ (1 if (i // 8) % 2 else 16)) for i in range(32)]
    route_after = [(i, i ^ (16 if (i // 8) % 2 else 1)) for i in range(32)]
    rows, wide = half_rows // 8, heads * HEAD_DIM

    def block(chunk, dtype=jnp.bfloat16):
        return shape((rows * len(chunk), wide), dtype)

    early = [(1, 1, chunk) for chunk in TRAVEL[:EARLY]]
    late = [(1, 1, chunk) for chunk in TRAVEL[EARLY:]] + [(1, 0, chunk) for chunk in STAY]
    unrot, *sends = call(
        functools.partial(send_kernel, early),
        [shape((2, tokens, wide), jnp.bfloat16)] + [block(chunk[2]) for chunk in early],
        [VMEM] * 12,
        work,
    )(stats, other, *near, *across, cosine, sine, own, far)
    everywhere = sum(TRAVEL, ())
    late.append((0, 1, everywhere))
    *more, turn_keep = call(
        functools.partial(rest_kernel, late),
        [block(chunk[2]) for chunk in late[:-1]] + [block(everywhere, jnp.float32)],
        [VMEM] * 3,
        work,
    )(own, far, unrot)
    sends += more
    (stay_keep,) = call(
        functools.partial(rest_kernel, [(0, 0, everywhere)]),
        [block(everywhere, jnp.float32)],
        [VMEM] * 3,
        work,
    )(own, far, unrot)
    come = []
    for send in sends:
        come.append(lax.ppermute(send, BOTH, route))
    totals = []
    for number, chunk in enumerate(TRAVEL):
        first = everywhere.index(chunk[0])
        send = call(
            functools.partial(add_kernel, rows * first), block(chunk), [VMEM] * 2, 1 << 20
        )(turn_keep, come[number])
        arrived = lax.ppermute(send, BOTH, route_after)
        kernel, outs = total_kernel, [block((distance,)) for distance in chunk]
        if 0 in chunk:
            split = [shape((out_rows, wide), jnp.bfloat16)] * 2
            kernel, outs = last_total_kernel, split + [block((0,), jnp.float32)]
        source = next(i for i, other in enumerate(STAY) if chunk[0] in other)
        inside = STAY[source].index(chunk[0])
        totals += call(
            functools.partial(kernel, rows * first, rows * inside),
            outs,
            [VMEM] * 3,
            1 << 20,
        )(stay_keep, come[len(TRAVEL) + source], arrived)
    *sends, cross, mine = totals
    arrived = []
    for distance, send in zip(everywhere, sends):
        along = [(i, (i + 2 * distance) % 8) for i in range(8)]
        arrived.append(lax.ppermute(send, "fsdp", along))
    across = [(i, (i // 8 ^ 1) * 8 + (i + 6) % 8) for i in range(32)]
    cross = lax.ppermute(cross, BOTH, across)
    columns = shape((out_rows, wide), jnp.float32)
    here, there = call(last_kernel, [columns] * 2, [VMEM] * 3, 1 << 20)(mine, *arrived[:2])
    there = swapped(there, "blk", 1)
    return call(
        functools.partial(next_kernel, (1.0 - decay_rate) / lax.axis_size("fsdp")),
        shape(hessian.shape, jnp.float32),
        [VMEM] * 5,
        1 << 20,
    )(here, arrived[2], there, cross, hessian)


def reduced_anywhere(normed, picked, queries, key_states, values, cotangent):
    rows, tokens = queries.shape[0], key_states.shape[0]
    size, blk = lax.axis_size("blk"), lax.axis_index("blk")
    every_query = lax.all_gather(queries, "blk", axis=0)
    every_cot = lax.all_gather(cotangent, "blk", axis=0)
    order = jnp.arange(size, dtype=jnp.int32)
    ids = order[:, None]
    reach = jnp.where(
        ids == blk, picked, jnp.where(ids > blk, jnp.int32(tokens), jnp.int32(-1))
    ).reshape(1, size * rows)
    reach = jnp.tile(reach, (1, chunks(size * rows)[0]))
    cosine, sine = lax.dynamic_index_in_dim(
        rotation_rows(np.arange(size * tokens)).reshape(2, size, tokens, HEAD_DIM), blk, 1, False
    )
    stats, expo, grads, query = attention_stats(
        functools.partial(any_stats_kernel, size),
        [every_query[i] for i in range(size)],
        [every_cot[i] for i in range(size)],
        [key_states],
        [values],
        (reach,),
        KV_HEADS,
    )
    gathered = lax.all_gather(stats, "blk", axis=0)
    others = [gathered[(blk + i) % size] for i in range(1, size)]
    unrotated = call(
        functools.partial(grad_kernel, size),
        shape((tokens, KV_HEADS * HEAD_DIM), jnp.bfloat16),
        [VMEM] * (size + 5),
        1 << 28,
    )(stats, *others, expo, grads, query, cosine, sine)
    term = lax.dot_general(
        normed, unrotated, (((0,), (0,)), ((), ())), preferred_element_type=jnp.float32
    )
    return lax.psum_scatter(term, BOTH, scatter_dimension=0, tiled=True)


def on_torus(blocks, sequences):
    return blocks == 4 and sequences == 8


def local(normed, picked, queries, key_states, values, cotangent, hessian):
    given = (normed[0], picked, queries[0], key_states[0], values[0], cotangent[0])
    rows, tokens, out_rows = queries.shape[1], key_states.shape[1], hessian.shape[0]
    blocks, sequences = lax.axis_size("blk"), lax.axis_size("fsdp")
    fits = rows & (rows - 1) == 0 and rows <= 16 and tokens % 128 == 0 and out_rows % 16 == 0
    if on_torus(blocks, sequences):
        assert fits
        return reduced_on_torus(*given, hessian)
    summed = reduced_anywhere(*given)
    return decay_rate * hessian + (1.0 - decay_rate) * summed * summed / sequences


def solution(mesh):
    placed = (
        P("fsdp", "blk", None),
        P("fsdp", "blk"),
        P("fsdp", "blk", None),
        P("fsdp", "blk", None),
        P("fsdp", "blk", None),
        P("fsdp", "blk", None),
        P(("blk", "fsdp"), None),
    )
    return jax.shard_map(
        local, mesh=mesh, in_specs=placed, out_specs=P(("blk", "fsdp"), None), check_vma=False
    )
```
